512 devices in a mesh: grp: 8 (over x, core), sub: 64 (over z, y).
Axes of the slice: x: 4, y: 8, z: 8, core: 2. Of those that a mesh axis runs over, the one named last changes fastest.
Arguments:
- overall_quantity_unnormalized: float32 [16, 64, 1024, 128], P(None, 'grp', 'sub'), may hold values from 0.05 to 1
- reservoir_pressure_field: float32 [64, 1024, 128], P('grp', 'sub'), may hold values from 0.7 to 1.3
- reservoir_heat_level: float32 [64, 1024, 128], P('grp', 'sub'), may hold values from 0.9 to 1.2
- condensed_flag: int32 [64, 1024, 128], P('grp', 'sub'), may hold values 0 or 1
- permeability_field: float32 [64, 1024, 128], P('grp', 'sub'), may hold values from 0.1 to 10
- pore_capacity: float32 [64, 1024, 128], P('grp', 'sub'), may hold values from 0.05 to 0.3
- former_chemical_quantity: float32 [16, 64, 1024, 128], P(None, 'grp', 'sub'), may hold values from 0 to 0.03
- transmissibility_multipliers: float32 [3], replicated, may hold values from 0.3 to 3
- viscosity_pair: float32 [2], replicated, may hold values from 0.3 to 3
- crit_kelvin_values: float32 [16], replicated, may hold values from 0.3 to 2.5
- attraction_parameters: float32 [16], replicated, may hold values from 0.3 to 4
- repulsive_parameters: float32 [16], replicated, may hold values from 0.02 to 0.15
- attraction_thermal_gradients: float32 [16], replicated, may hold values from 0.3 to 1.2
- binary_coupling_matrix: float32 [16, 16], replicated, may hold values from 0 to 0.3, as said below
- injected_recipe_unnormalized: float32 [16], replicated, may hold values from 0.05 to 1
- perforated_locale: int32 [131072], P(('grp', 'sub')), may hold values from 0 to 16383
- perforated_member: int32 [131072, 1], P(('grp', 'sub')), may hold values from 0 to 63; in each aligned block of 256 rows (0 to 255, 256 to 511, ...) at most 10 rows name the same one
- connection_conduit_piece: int32 [131072], P(('grp', 'sub')), may hold values from 0 to 31
- connection_inflow_strength: float32 [131072], P(('grp', 'sub')), may hold values from 0.02 to 0.2
- group_member_place: int32 [8, 64], P('grp'), may hold values from 0 to 63, each once within a row
- conduit_pieces_toe_forward: int32 [512, 32], P(('grp', 'sub')), may hold values from 0 to 31, each once within a row
- conduit_piece_pressures: float32 [512, 32], P(('grp', 'sub')), may hold values from 0.7 to 1.3
- downstream_exit_pressure: float32 [512], P(('grp', 'sub')), may hold values from 0.6 to 1.2
- friction_factors: float32 [512], P(('grp', 'sub')), may hold values from 3.0517578e-05 to 0.00030517578
Outputs:
- residual: float32 [16, 64, 1024, 128], P(None, 'grp', 'sub')
- ln_phi: bfloat16 [16, 64, 1024, 128], P(None, 'grp', 'sub')
- well_residual: float32 [512, 32], P(('grp', 'sub'))
The draws below stay inside these ranges and needn't reach their ends.
Inputs may be any that keep to these rules, and one draw needn't show every extreme that they name: `perforated_locale`: flattened index (first, second, layer) of a cell of the listing device's own block. `perforated_member`: a well of the listing device's group; among the 256 rows of one device at most 10 name the same well. `group_member_place`: each row is a permutation; slot j of a group lies on the group's device j. `conduit_pieces_toe_forward`: each row is a permutation of the segments. `binary_coupling_matrix`: symmetric with zero diagonal.
All inputs are finite; a program needn't handle non-finite values. No bound on the sum of `condensed_flag` on one device may be relied on, other than what follows from the above.
Results may differ from the reference program's by a relative error of at most 0.001.
Values sent between devices are 32-bit elements; how exact they have to be, the bound alone decides.
A program may use at most 64 MiB of HBM per device.

```python
import math
import jax
import jax.numpy as jnp
import numpy as np
from jax import lax

CHEMICAL_KINDS = 16
CX = 8
CY = 16
STRATA_NUMBER = 128
NEWT = 8
PERF_DEV = 256
SEGS = 32
GRID_NX_EXTENT = 64
GRID_NY_EXTENT = 1024
WELL_G = 64
WELLS = 512
CAP = 10
N_GRP = 8
N_SUB = 64
DEVICES = 512


def draw_binary_coupling_matrix(key, part):
    values = jax.random.uniform(key, (CHEMICAL_KINDS, CHEMICAL_KINDS), jnp.float32, 0.0, 0.3)
    both = 0.5 * (values + values.T)
    return both * (1.0 - jnp.eye(CHEMICAL_KINDS, dtype=jnp.float32))


def place_ends(values, rng, low, high):
    longest = values.shape.index(max(values.shape))
    spots = []
    for shift in (0, 1):
        where = [jax.random.randint(jax.random.fold_in(rng, axis), (), 0, length) for axis, length in enumerate(values.shape)]
        where[longest] = (where[longest] + shift) % values.shape[longest]
        spots.append(tuple(where))
    return values.at[spots[0]].set(low).at[spots[1]].set(high)


def level_of(own_key, extent, pieces, low, high):
    loudness, own = 1.0, jax.random.fold_in(own_key, 6)
    for dim, shards_of in pieces:
        heights = jnp.exp(jax.random.uniform(jax.random.fold_in(own, dim), (shards_of,), jnp.float32, low / len(pieces), high / len(pieces)))
        loudness = loudness * jnp.repeat(heights, extent[dim] // shards_of).reshape([-1 if axis == dim else 1 for axis in range(len(extent))])
    return loudness


def assign_block(rng, own, number, rows, number_of, top, reach, skew):
    sequence = jax.random.permutation(rng, number_of)
    heavy_load, common = shares(number_of, rows * top, reach, skew, True), shares(number_of, rows * top, reach, skew, False)
    places = jnp.arange(number_of)

    def named(sizes, offset_by):
        used = int((sizes > 0).sum())
        fixed = max(1, used // 4)
        passed = fixed + (places - fixed + offset_by * (used - fixed)) % max(1, number_of - fixed)
        return jnp.zeros((number_of,), jnp.int32).at[sequence[jnp.where(places < fixed, places, passed)]].set(jnp.asarray(sizes, jnp.int32))

    sizes = jnp.where(number % 4 == 0, named(heavy_load, number // 4), named(common, number - number // 4 - 1))
    mixed = jax.random.permutation(jax.random.fold_in(own, 3), number_of)
    giver, taker = mixed[0:number_of // 2 * 2:2], mixed[1:number_of // 2 * 2:2]
    margin = jnp.minimum(sizes[giver] - 1, reach - sizes[taker]) // 2
    margin = jnp.where((giver == sequence[0]) | (taker == sequence[0]) | (sizes[taker] == 0), 0, jnp.maximum(margin, 0))
    passed = jax.random.randint(jax.random.fold_in(own, 4), (number_of // 2,), 0, 1 << 20) % (margin + 1)
    sizes = sizes.at[giver].add(-passed).at[taker].add(passed)
    members = jnp.searchsorted(jnp.cumsum(sizes), jnp.arange(rows * top), side="right").astype(jnp.int32)
    listing = members.reshape(top, rows).T
    listing = listing[jax.random.permutation(jax.random.fold_in(own, 1), rows)]
    offset_by = jax.random.randint(jax.random.fold_in(own, 2), (rows, 1), 0, top)
    return jnp.take_along_axis(listing, (jnp.arange(top)[None, :] + offset_by) % top, axis=1)


def shares(number_of, total, reach, lean, full):
    portions = [(1 << 20) // math.isqrt(standing ** lean) + 1 for standing in range(1, number_of + 1)]
    largest = reach if full else min(reach, max(-(-total // number_of), total * portions[0] // sum(portions)))
    least = 1 if total - largest >= number_of - 1 else 0
    counts, rest = [largest] + [least] * (number_of - 1), total - largest - least * (number_of - 1)
    while rest > 0:
        candidates = [i for i in range(1, number_of) if counts[i] < largest] or [i for i in range(1, number_of) if counts[i] < reach]
        whole, left = sum([portions[i] for i in candidates]), rest
        for i in candidates:
            more = min(reach - counts[i], max(1, left * portions[i] // whole), rest)
            counts[i] = counts[i] + more
            rest = rest - more
    return np.array(counts)


def setup_inputs(seed: int = 0) -> dict:
    streams_of = jax.random.split(jax.random.key(seed), 25)
    overall_quantity_unnormalized = jnp.clip(jnp.exp(math.log(1.0) - 2.9957323 * jax.random.uniform(streams_of[0], (CHEMICAL_KINDS, GRID_NX_EXTENT, GRID_NY_EXTENT, STRATA_NUMBER), jnp.float32) ** level_of(streams_of[0], (CHEMICAL_KINDS, GRID_NX_EXTENT, GRID_NY_EXTENT, STRATA_NUMBER), ((1, 8), (2, 64)), -0.2, 0.2)), 0.05, 1.0)
    reservoir_pressure_field = jnp.clip(0.7 + 0.59999996 * jax.random.uniform(streams_of[1], (GRID_NX_EXTENT, GRID_NY_EXTENT, STRATA_NUMBER), jnp.float32) ** level_of(streams_of[1], (GRID_NX_EXTENT, GRID_NY_EXTENT, STRATA_NUMBER), ((0, 8), (1, 64)), -0.2, 0.2), 0.7, 1.3)
    reservoir_heat_level = jnp.clip(0.9 + 0.30000007 * jax.random.uniform(streams_of[2], (GRID_NX_EXTENT, GRID_NY_EXTENT, STRATA_NUMBER), jnp.float32) ** level_of(streams_of[2], (GRID_NX_EXTENT, GRID_NY_EXTENT, STRATA_NUMBER), ((0, 8), (1, 64)), -0.2, 0.2), 0.9, 1.2)
    condensed_flag = place_ends((jax.random.randint(streams_of[3], (GRID_NX_EXTENT, GRID_NY_EXTENT, STRATA_NUMBER), 0, 2) < 1).astype(jnp.int32), jax.random.fold_in(streams_of[3], 1), 0, 1)
    permeability_field = jnp.clip(jnp.exp(math.log(10.0) - 4.6051702 * jax.random.uniform(streams_of[4], (GRID_NX_EXTENT, GRID_NY_EXTENT, STRATA_NUMBER), jnp.float32) ** level_of(streams_of[4], (GRID_NX_EXTENT, GRID_NY_EXTENT, STRATA_NUMBER), ((0, 8), (1, 64)), -0.2, 0.2)), 0.1, 10.0)
    pore_capacity = jnp.clip(jnp.exp(math.log(0.3) - 1.7917595 * jax.random.uniform(streams_of[5], (GRID_NX_EXTENT, GRID_NY_EXTENT, STRATA_NUMBER), jnp.float32) ** level_of(streams_of[5], (GRID_NX_EXTENT, GRID_NY_EXTENT, STRATA_NUMBER), ((0, 8), (1, 64)), -0.2, 0.2)), 0.05, 0.3)
    former_chemical_quantity = jnp.clip(0.03 * jax.random.uniform(streams_of[6], (CHEMICAL_KINDS, GRID_NX_EXTENT, GRID_NY_EXTENT, STRATA_NUMBER), jnp.float32) ** level_of(streams_of[6], (CHEMICAL_KINDS, GRID_NX_EXTENT, GRID_NY_EXTENT, STRATA_NUMBER), ((1, 8), (2, 64)), -0.2, 0.2), 0.0, 0.03)
    transmissibility_multipliers = jnp.clip(jnp.exp(jax.random.uniform(streams_of[7], (3,), jnp.float32, math.log(0.3), math.log(3.0))), 0.3, 3.0)
    viscosity_pair = jnp.clip(jnp.exp(jax.random.uniform(streams_of[8], (2,), jnp.float32, math.log(0.3), math.log(3.0))), 0.3, 3.0)
    crit_kelvin_values = jnp.clip(jnp.exp(jax.random.uniform(streams_of[9], (CHEMICAL_KINDS,), jnp.float32, math.log(0.3), math.log(2.5))), 0.3, 2.5)
    attraction_parameters = jnp.clip(jnp.exp(jax.random.uniform(streams_of[10], (CHEMICAL_KINDS,), jnp.float32, math.log(0.3), math.log(4.0))), 0.3, 4.0)
    repulsive_parameters = jnp.clip(jnp.exp(jax.random.uniform(streams_of[11], (CHEMICAL_KINDS,), jnp.float32, math.log(0.02), math.log(0.15))), 0.02, 0.15)
    attraction_thermal_gradients = jnp.clip(jax.random.uniform(streams_of[12], (CHEMICAL_KINDS,), jnp.float32, 0.3, 1.2), 0.3, 1.2)
    binary_coupling_matrix = draw_binary_coupling_matrix(jax.random.fold_in(streams_of[24], 71), 0)
    injected_recipe_unnormalized = jnp.clip(jnp.exp(jax.random.uniform(streams_of[14], (CHEMICAL_KINDS,), jnp.float32, math.log(0.05), math.log(1.0))), 0.05, 1.0)
    perforated_locale = place_ends(jax.random.randint(streams_of[15], (DEVICES * PERF_DEV,), 0, CX * CY * STRATA_NUMBER), jax.random.fold_in(streams_of[15], 1), 0, (CX * CY * STRATA_NUMBER) - 1).astype(jnp.int32)
    perforated_member_keys = jax.random.split(jax.random.fold_in(streams_of[16], 1), (DEVICES * PERF_DEV) // PERF_DEV)
    perforated_member_turns = jax.random.permutation(jax.random.fold_in(streams_of[16], 3), (DEVICES * PERF_DEV) // PERF_DEV)
    perforated_member = jax.vmap(lambda own, number: assign_block(jax.random.fold_in(streams_of[16], 2), own, number, PERF_DEV, WELL_G, 1, CAP, 2))(perforated_member_keys, perforated_member_turns).reshape((DEVICES * PERF_DEV, 1))
    connection_conduit_piece = place_ends(jax.random.randint(streams_of[17], (DEVICES * PERF_DEV,), 0, SEGS), jax.random.fold_in(streams_of[17], 1), 0, SEGS - 1).astype(jnp.int32)
    connection_inflow_strength = jnp.clip(jnp.exp(math.log(0.2) - 2.3025851 * jax.random.uniform(streams_of[18], (DEVICES * PERF_DEV,), jnp.float32) ** level_of(streams_of[18], (DEVICES * PERF_DEV,), ((0, 512),), -0.2, 0.2)), 0.02, 0.2)
    group_member_place = jax.vmap(lambda own: jax.random.permutation(own, WELL_G))(jax.random.split(streams_of[19], N_GRP)).reshape((N_GRP, WELL_G)).astype(jnp.int32)
    conduit_pieces_toe_forward = jax.vmap(lambda own: jax.random.permutation(own, SEGS))(jax.random.split(streams_of[20], WELLS)).reshape((WELLS, SEGS)).astype(jnp.int32)
    conduit_piece_pressures = jnp.clip(0.7 + 0.59999996 * jax.random.uniform(streams_of[21], (WELLS, SEGS), jnp.float32) ** level_of(streams_of[21], (WELLS, SEGS), ((0, 512),), -0.2, 0.2), 0.7, 1.3)
    downstream_exit_pressure = jnp.clip(0.6 + 0.6 * jax.random.uniform(streams_of[22], (WELLS,), jnp.float32) ** level_of(streams_of[22], (WELLS,), ((0, 512),), -0.2, 0.2), 0.6, 1.2)
    friction_factors = jnp.clip(jnp.exp(math.log(0.00030517578) - 2.3025851 * jax.random.uniform(streams_of[23], (WELLS,), jnp.float32) ** level_of(streams_of[23], (WELLS,), ((0, 512),), -0.2, 0.2)), 3.0517578125e-05, 0.00030517578)
    return dict(overall_quantity_unnormalized=overall_quantity_unnormalized, reservoir_pressure_field=reservoir_pressure_field, reservoir_heat_level=reservoir_heat_level, condensed_flag=condensed_flag, permeability_field=permeability_field, pore_capacity=pore_capacity, former_chemical_quantity=former_chemical_quantity, transmissibility_multipliers=transmissibility_multipliers, viscosity_pair=viscosity_pair, crit_kelvin_values=crit_kelvin_values, attraction_parameters=attraction_parameters, repulsive_parameters=repulsive_parameters, attraction_thermal_gradients=attraction_thermal_gradients, binary_coupling_matrix=binary_coupling_matrix, injected_recipe_unnormalized=injected_recipe_unnormalized, perforated_locale=perforated_locale, perforated_member=perforated_member, connection_conduit_piece=connection_conduit_piece, connection_inflow_strength=connection_inflow_strength, group_member_place=group_member_place, conduit_pieces_toe_forward=conduit_pieces_toe_forward, conduit_piece_pressures=conduit_piece_pressures, downstream_exit_pressure=downstream_exit_pressure, friction_factors=friction_factors)


ROOT_TWO = math.sqrt(2.0)

def gas_oil_partition(overall_quantity_unnormalized, reservoir_pressure_field, reservoir_heat_level, condensed_flag, crit_kelvin_values, attraction_parameters, repulsive_parameters, attraction_thermal_gradients, binary_coupling_matrix, viscosity_pair):
    shape = overall_quantity_unnormalized.shape
    replicate_across = (slice(None),) + (None,) * (len(shape) - 1)
    chemical_labels = overall_quantity_unnormalized / lax.optimization_barrier(jnp.sum(overall_quantity_unnormalized, axis=0))
    thermal_adjuster = (1.0 + attraction_thermal_gradients[replicate_across] * (1.0 - jnp.sqrt(reservoir_heat_level / crit_kelvin_values[replicate_across]))) ** 2
    blended_attraction = attraction_parameters[replicate_across] * thermal_adjuster * reservoir_pressure_field / (reservoir_heat_level * reservoir_heat_level)
    roots = jnp.sqrt(blended_attraction)
    mixture_excluded_volume = repulsive_parameters[replicate_across] * reservoir_pressure_field / reservoir_heat_level
    mixed = jnp.dot(1.0 - binary_coupling_matrix, (roots * chemical_labels).reshape(shape[0], -1), precision=lax.Precision.HIGHEST).reshape(shape)
    psi = roots * mixed
    big_a = lax.optimization_barrier(jnp.sum(chemical_labels * psi, axis=0))
    big_b = lax.optimization_barrier(jnp.sum(chemical_labels * mixture_excluded_volume, axis=0))
    deviation_zvalue = jnp.where(condensed_flag == 1, big_b + 0.01, 1.0 + big_b)
    lin_c2 = big_b - 1.0
    lin_c1 = big_a - 3.0 * big_b * big_b - 2.0 * big_b
    lin_c0 = big_b * big_b + big_b * big_b * big_b - big_a * big_b
    for step in range(NEWT):
        value = ((deviation_zvalue + lin_c2) * deviation_zvalue + lin_c1) * deviation_zvalue + lin_c0
        slope = (3.0 * deviation_zvalue + 2.0 * lin_c2) * deviation_zvalue + lin_c1
        deviation_zvalue = jnp.maximum(deviation_zvalue - value / jnp.maximum(slope, 0.1), big_b + 0.01)
    ratio = jnp.log((deviation_zvalue + (1.0 + ROOT_TWO) * big_b) / (deviation_zvalue + (1.0 - ROOT_TWO) * big_b))
    natural_log_activity = mixture_excluded_volume / big_b * (deviation_zvalue - 1.0) - jnp.log(deviation_zvalue - big_b) - (psi / (ROOT_TWO * big_b) - big_a * mixture_excluded_volume / (2.0 * ROOT_TWO * big_b * big_b)) * ratio
    blended_dilution_ratio = reservoir_pressure_field / (deviation_zvalue * reservoir_heat_level)
    visc = jnp.where(condensed_flag == 1, viscosity_pair[1], viscosity_pair[0])
    relative_flow_ease = blended_dilution_ratio / visc
    return (chemical_labels, natural_log_activity, blended_dilution_ratio, relative_flow_ease)

def face(c_a, p_a, k_a, c_b, p_b, k_b, factor):
    trans = factor * 2.0 * k_a * k_b / (k_a + k_b)
    return trans * (p_a - p_b) * jnp.where(p_a > p_b, c_a, c_b)

def shifted(arr, axis, upward):
    width = [(0, 0)] * arr.ndim
    width[axis] = (1, 1)
    padded = jnp.pad(arr, width)
    size = arr.shape[axis]
    start = 2 if upward else 0
    return lax.slice_in_dim(padded, start, start + size, axis=arr.ndim + axis if axis < 0 else axis)

def reference(overall_quantity_unnormalized, reservoir_pressure_field, reservoir_heat_level, condensed_flag, permeability_field, pore_capacity, former_chemical_quantity, transmissibility_multipliers, viscosity_pair, crit_kelvin_values, attraction_parameters, repulsive_parameters, attraction_thermal_gradients, binary_coupling_matrix, injected_recipe_unnormalized, perforated_locale, perforated_member, connection_conduit_piece, connection_inflow_strength, group_member_place, conduit_pieces_toe_forward, conduit_piece_pressures, downstream_exit_pressure, friction_factors):
    species_share = jnp.moveaxis(overall_quantity_unnormalized, 0, 1)
    earlier_share = jnp.moveaxis(former_chemical_quantity, 0, 1)

    def stratum_plane(items):
        crude_sample, pressure_level, kelvin_level, label_vector, pore, old = items
        chemical_labels, natural_log_activity, blended_dilution_ratio, relative_flow_ease = gas_oil_partition(crude_sample, pressure_level, kelvin_level, label_vector, crit_kelvin_values, attraction_parameters, repulsive_parameters, attraction_thermal_gradients, binary_coupling_matrix, viscosity_pair)
        storage_term = pore * blended_dilution_ratio * chemical_labels - old
        return (chemical_labels, natural_log_activity, relative_flow_ease, storage_term)
    chemical_labels, natural_log_activity, relative_flow_ease, storage_term = lax.map(stratum_plane, (species_share, reservoir_pressure_field, reservoir_heat_level, condensed_flag, pore_capacity, earlier_share))
    carried = relative_flow_ease[:, None] * chemical_labels
    carried_pad = jnp.pad(carried, ((1, 1), (0, 0), (0, 0), (0, 0)))
    press_pad = jnp.pad(reservoir_pressure_field, ((1, 1), (0, 0), (0, 0)))
    perm_pad = jnp.pad(permeability_field, ((1, 1), (0, 0), (0, 0)))

    def slab_flux(index):
        cwin = lax.dynamic_slice_in_dim(carried_pad, index, 3, 0)
        pwin = lax.dynamic_slice_in_dim(press_pad, index, 3, 0)
        kwin = lax.dynamic_slice_in_dim(perm_pad, index, 3, 0)
        c_a, p_a, k_a = (cwin[1], pwin[1], kwin[1])
        total = lax.dynamic_index_in_dim(storage_term, index, 0, keepdims=False)
        total = total + face(c_a, p_a, k_a, cwin[2], pwin[2], kwin[2], transmissibility_multipliers[0])
        total = total + face(c_a, p_a, k_a, cwin[0], pwin[0], kwin[0], transmissibility_multipliers[0])
        for axis, factor in ((0, transmissibility_multipliers[1]), (1, transmissibility_multipliers[2])):
            for upward in (True, False):
                total = total + face(c_a, p_a, k_a, shifted(c_a, axis - 2, upward), shifted(p_a, axis - 2, upward), shifted(k_a, axis - 2, upward), factor)
        return total
    resid_x = lax.map(slab_flux, jnp.arange(GRID_NX_EXTENT, dtype=jnp.int32))
    rows = jnp.arange(N_GRP * N_SUB * PERF_DEV, dtype=jnp.int32)
    device = rows // PERF_DEV
    grp_index = device // N_SUB
    sub_index = device % N_SUB
    cell_x = grp_index * CX + perforated_locale // (CY * STRATA_NUMBER)
    cell_y = sub_index * CY + perforated_locale // STRATA_NUMBER % CY
    cell_z = perforated_locale % STRATA_NUMBER
    p_cell = reservoir_pressure_field[cell_x, cell_y, cell_z]
    m_cell = relative_flow_ease[cell_x, cell_y, cell_z]
    z_cell = chemical_labels[cell_x, :, cell_y, cell_z].T
    slot = grp_index * WELL_G + group_member_place[grp_index, perforated_member[:, 0]]
    p_seg = conduit_piece_pressures[slot, connection_conduit_piece]
    drop = p_cell - p_seg
    injected = injected_recipe_unnormalized / jnp.sum(injected_recipe_unnormalized)
    inflow = (connection_inflow_strength * m_cell * drop)[None, :] * jnp.where(drop[None, :] > 0, z_cell, injected[:, None])
    resid_x = resid_x.at[cell_x, :, cell_y, cell_z].add(inflow.T)
    residual = jnp.moveaxis(resid_x, 1, 0)
    ln_phi = jnp.moveaxis(natural_log_activity, 1, 0).astype(jnp.bfloat16)
    totals = lax.optimization_barrier(jnp.sum(inflow, axis=0))
    rate = jax.ops.segment_sum(totals, slot * SEGS + connection_conduit_piece, num_segments=WELLS * SEGS).reshape(WELLS, SEGS)
    ordered = jnp.take_along_axis(rate, conduit_pieces_toe_forward, axis=1)
    running = jnp.cumsum(ordered, axis=1)
    press_ord = jnp.take_along_axis(conduit_piece_pressures, conduit_pieces_toe_forward, axis=1)
    nexts = jnp.concatenate([press_ord[:, 1:], downstream_exit_pressure[:, None]], axis=1)
    res_ord = press_ord - nexts - friction_factors[:, None] * running * jnp.abs(running)
    well_rows = jnp.arange(WELLS, dtype=jnp.int32)[:, None]
    well_residual = jnp.zeros((WELLS, SEGS), jnp.float32).at[well_rows, conduit_pieces_toe_forward].set(res_ord)
    return (residual, ln_phi, well_residual)
```

```python
import functools
import math

import jax
import jax.numpy as jnp
from jax import lax
from jax.experimental import pallas as pl
from jax.experimental.pallas import tpu as pltpu
from jax.sharding import PartitionSpec as P

NEWT = 8
ROOT_TWO = math.sqrt(2.0)
MESH = pl.DeviceIdType.MESH
NC = 16
CX = 8
CY = 16
LANES = 128
LINE = 8
SMALL = 15
SCALARS = 8
F32 = jnp.float32
BF16 = jnp.bfloat16
HIGHEST = lax.Precision.HIGHEST


def iota(shape, axis):
    return lax.broadcasted_iota(jnp.int32, shape, axis)


def hot(index_row, rows):
    mask = iota((rows, index_row.shape[1]), 0) == index_row
    return jnp.where(mask, 1.0, 0.0).astype(F32)


def pieces_of(x, count):
    out = []
    for _ in range(count):
        top = x.astype(BF16)
        out.append(top)
        x = x - top.astype(F32)
    return out


def mm(a, b):
    return lax.dot_general(a, b, (((1,), (0,)), ((), ())), preferred_element_type=F32)


def mm_nt(a, b):
    return lax.dot_general(a, b, (((1,), (1,)), ((), ())), preferred_element_type=F32)


def mm_full(a, b):
    return lax.dot_general(
        a, b, (((1,), (0,)), ((), ())), precision=HIGHEST, preferred_element_type=F32
    )


def mm_full_nt(a, b):
    return lax.dot_general(
        a, b, (((1,), (1,)), ((), ())), precision=HIGHEST, preferred_element_type=F32
    )


def pick_rows(field, lane_hot, row_mask, count):
    parts = pieces_of(field, count)
    found = mm(jnp.concatenate(parts, axis=0), lane_hot)
    rows = field.shape[0]
    total = found[:rows]
    for i in range(1, count):
        total = total + found[i * rows : (i + 1) * rows]
    return jnp.sum(jnp.where(row_mask, total, 0.0), axis=0, keepdims=True)


def body(
    n_grp,
    n_sub,
    n_hbm,
    p_hbm,
    t_hbm,
    flag_hbm,
    k_hbm,
    pore_hbm,
    old_hbm,
    *refs,
):
    small_hbm, refs = refs[:SMALL], refs[SMALL:]
    exit_p, friction, *refs = refs
    resid_ref, lnphi_ref, well_ref = refs[:3]
    small_refs, refs = refs[3 : 3 + SMALL], refs[3 + SMALL :]
    (
        trans,
        visc,
        crit,
        attract,
        covol,
        kappa,
        kij,
        recipe,
        loc_ref,
        mem_ref,
        seg_ref,
        wi_ref,
        gmp_ref,
        order_ref,
        cpp_ref,
    ) = small_refs
    (
        n_v,
        t_v,
        flag_v,
        pore_v,
        old_v,
        st,
        um_v,
        w_v,
        mob_v,
        e1_v,
        e2_v,
        e3_v,
        pv_v,
        wp_v,
        wn_v,
        c0_t,
        c1_t,
        cb_t,
        inj_t,
        row_v,
        ag1_src,
        ag1,
        ag2_src,
        ag2,
        rs1_src,
        rs1,
        rs2_src,
        rs2,
        ys_lo,
        ys_hi,
        yr_lo,
        yr_hi,
        in_sem,
        send_sem,
        recv_sem,
        halo_send,
        halo_recv,
        small_sem,
    ) = refs
    g = lax.axis_index("grp")
    s = lax.axis_index("sub")
    z, y = s // LINE, s % LINE

    def z_peer(d):
        return {"sub": ((z + d) % LINE) * LINE + y}

    def y_peer(d):
        return {"sub": z * LINE + (y + d) % LINE}

    g_up, g_down = {"grp": (g + 1) % n_grp}, {"grp": (g + n_grp - 1) % n_grp}
    s_up, s_down = {"sub": (s + 1) % n_sub}, {"sub": (s + n_sub - 1) % n_sub}

    inner = pl.ds(1, CX)
    rows = pl.ds(8, CY)
    half = CX // 2
    loads = [
        pltpu.make_async_copy(t_hbm, t_v, in_sem.at[0]),
        pltpu.make_async_copy(p_hbm, st.at[NC, inner, rows], in_sem.at[1]),
        pltpu.make_async_copy(n_hbm.at[:, pl.ds(0, half)], n_v.at[:, pl.ds(0, half)], in_sem.at[2]),
        pltpu.make_async_copy(
            n_hbm.at[:, pl.ds(half, half)], n_v.at[:, pl.ds(half, half)], in_sem.at[3]
        ),
        pltpu.make_async_copy(flag_hbm, flag_v, in_sem.at[4]),
        pltpu.make_async_copy(k_hbm, st.at[NC + 1, inner, rows], in_sem.at[5]),
        pltpu.make_async_copy(pore_hbm, pore_v, in_sem.at[6]),
        pltpu.make_async_copy(old_hbm, old_v, in_sem.at[7]),
    ]
    small_loads = [
        pltpu.make_async_copy(src, dst, small_sem.at[i])
        for i, (src, dst) in enumerate(zip(small_hbm, small_refs))
    ]
    for load in small_loads + loads:
        load.start()

    barrier = pltpu.get_barrier_semaphore()
    peers = [z_peer(d) for d in range(1, LINE)] + [y_peer(d) for d in range(1, LINE)]
    peers += [g_up, g_down, s_up, s_down]
    for peer in peers:
        pl.semaphore_signal(barrier, inc=1, device_id=peer, device_id_type=MESH)

    for load in small_loads:
        load.wait()

    tile = (8, LANES)
    total = jnp.zeros(tile, F32)
    for i in range(NC):
        total = total + recipe[i]
    for i in range(NC):
        amount = jnp.sqrt(jnp.full(tile, attract[i], F32))
        slope = jnp.full(tile, kappa[i], F32)
        c0_t[i] = amount * (1.0 + slope)
        c1_t[i] = amount * slope / jnp.sqrt(jnp.full(tile, crit[i], F32))
        cb_t[i] = jnp.full(tile, covol[i], F32)
        inj_t[i] = jnp.full(tile, recipe[i], F32) / total

    row_v[...] = jnp.zeros(tile, F32)
    row_v[0:1, 0:32] = cpp_ref[...]
    own_row = row_v[0:1, :]
    ag1_src[...] = jnp.where(iota(tile, 0) == y, own_row, 0.0)

    loc = [loc_ref[h : h + 1, :] for h in range(2)]
    row_of = jnp.concatenate([v // LANES for v in loc], axis=1)
    lane_of = jnp.concatenate([v % LANES for v in loc], axis=1)
    member = jnp.concatenate([mem_ref[h : h + 1, :] for h in range(2)], axis=1)
    segment = jnp.concatenate([seg_ref[h : h + 1, :] for h in range(2)], axis=1)
    strength = jnp.concatenate([wi_ref[h : h + 1, :] for h in range(2)], axis=1)
    wells = n_sub
    place = jnp.where(iota((wells, wells), 0) == gmp_ref[...], 1.0, 0.0).astype(BF16)
    slot_hot = mm(place, hot(member, wells).astype(BF16))
    lane_hot = hot(lane_of, LANES)
    lane_hot_b = lane_hot.astype(BF16)
    row_mask = iota((LANES, 2 * LANES), 0) == row_of
    row_hot_b = jnp.where(row_mask, 1.0, 0.0).astype(BF16)
    seg_hot = hot(segment, LANES).astype(BF16)
    seg_hot_2 = hot(segment + 32, LANES).astype(BF16)

    order = jnp.where(iota((32, 32), 0) == order_ref[...], 1.0, 0.0).astype(F32)
    sub32, lane32 = iota((32, 32), 0), iota((32, 32), 1)
    upper = jnp.where(sub32 <= lane32, 1.0, 0.0).astype(F32)
    after = jnp.where(sub32 == lane32 + 1, 1.0, 0.0).astype(F32)
    before_hot = mm_full_nt(mm_full(order, upper), order)
    next_hot = mm_full_nt(mm_full(order, after), order)
    last_row = jnp.where(iota((8, 32), 1) == 31, 1.0, 0.0).astype(F32)
    last_hot = mm_full_nt(last_row, order)
    cpp = jnp.broadcast_to(cpp_ref[...], (8, 32))
    base = cpp - (mm_full(cpp, next_hot) + exit_p[0] * last_hot)

    loads[0].wait()
    loads[1].wait()
    loads[4].wait()
    loads[6].wait()

    def phase(b, _):
        xs = pl.ds(b * half, half)
        xp = pl.ds(b * half + 1, half)
        pltpu.make_async_copy(n_hbm.at[:, xs], n_v.at[:, xs], in_sem.at[2 + b]).wait()
        t = t_v[xs]
        p = st[NC, xp, rows, :]
        root_t = jnp.sqrt(t)
        whole = jnp.zeros_like(t)
        bsum = jnp.zeros_like(t)

        def wide(table, i):
            v = table[i]
            return jnp.broadcast_to(
                jnp.concatenate([v, v], axis=0)[None], (half, CY, LANES)
            )

        for i in range(NC):
            n = n_v[i, xs]
            u = jnp.abs(wide(c0_t, i) - wide(c1_t, i) * root_t)
            um_v[i, xs] = u
            w_v[i] = n * u
            whole = whole + n
            bsum = bsum + wide(cb_t, i) * n
        asum = jnp.zeros_like(t)
        for i in range(NC):
            m = None
            for j in range(NC):
                term = w_v[j] * (1.0 - kij[i, j])
                m = term if m is None else m + term
            um = um_v[i, xs] * m
            um_v[i, xs] = um
            asum = asum + n_v[i, xs] * um
        inv = 1.0 / whole
        inv_t = 1.0 / t
        pt = p * inv_t
        gain = pt * inv_t * inv
        big_a = gain * inv * asum
        big_b = pt * inv * bsum
        liquid = flag_v[xs] == 1
        zed = jnp.where(liquid, big_b + 0.01, 1.0 + big_b)
        low = big_b + 0.01
        c2 = big_b - 1.0
        c2x2 = 2.0 * c2
        c1 = big_a - 3.0 * big_b * big_b - 2.0 * big_b
        c0 = big_b * big_b + big_b * big_b * big_b - big_a * big_b
        for _step in range(NEWT):
            value = ((zed + c2) * zed + c1) * zed + c0
            slope = (3.0 * zed + c2x2) * zed + c1
            zed = jnp.maximum(zed - value / jnp.maximum(slope, 0.1), low)
        ratio = jnp.log((zed + (1.0 + ROOT_TWO) * big_b) / (zed + (1.0 - ROOT_TWO) * big_b))
        inv_b = 1.0 / big_b
        e3 = ratio * inv_b * (1.0 / ROOT_TWO)
        e1_v[xs] = pt * inv_b * ((zed - 1.0) + 0.5 * big_a * e3)
        e2_v[xs] = jnp.log(zed - big_b)
        e3_v[xs] = e3 * gain
        thick = jnp.where(liquid, visc[1], visc[0])
        mob = pt / (zed * thick)
        mob_v[xs] = mob
        pv_v[xs] = pore_v[xs] * thick
        share = mob * inv
        for i in range(NC):
            st[i, xp, rows, :] = n_v[i, xs] * share
        return 0

    lax.fori_loop(0, 2, phase, 0)

    pl.semaphore_wait(barrier, len(peers))

    def tile_copy(src, dst, kind, slot, peer):
        return pltpu.make_async_remote_copy(
            src_ref=src,
            dst_ref=dst,
            send_sem=send_sem.at[kind, slot],
            recv_sem=recv_sem.at[kind, slot],
            device_id=peer,
            device_id_type=MESH,
        )

    ag1_copies = [tile_copy(ag1_src, ag1.at[d], 0, d, y_peer(d)) for d in range(1, LINE)]
    for copy in ag1_copies:
        copy.start()

    p_cell = pick_rows(
        st[NC, inner, rows, :].reshape(LANES, LANES), lane_hot_b, row_mask, 3
    )
    mob_cell = pick_rows(mob_v[...].reshape(LANES, LANES), lane_hot_b, row_mask, 2)
    v0 = strength * mob_cell
    v1 = v0 * (p_cell - 1.0)
    left = jnp.concatenate([slot_hot * v0, slot_hot * v1], axis=1)
    right = jnp.concatenate([seg_hot, seg_hot_2], axis=1)
    sums = None
    for part in pieces_of(left, 3):
        found = mm_nt(part, right)
        sums = found if sums is None else sums + found
    rs1_src[...] = sums.reshape(LINE, LINE, LANES)
    rs1_copies = [
        tile_copy(rs1_src.at[(z + d) % LINE], rs1.at[d], 2, d, z_peer(d)) for d in range(1, LINE)
    ]
    for copy in rs1_copies:
        copy.start()

    loads[5].wait()

    def gather_rows(c, _):
        ys_lo[c] = st[c, inner, 8, :]
        ys_hi[c] = st[c, inner, 8 + CY - 1, :]
        return 0

    lax.fori_loop(0, NC + 2, gather_rows, 0)

    def halo_copy(src, dst, slot, peer):
        return pltpu.make_async_remote_copy(
            src_ref=src,
            dst_ref=dst,
            send_sem=halo_send.at[slot],
            recv_sem=halo_recv.at[slot],
            device_id=peer,
            device_id_type=MESH,
        )

    halo_copies = [
        halo_copy(st.at[:, CX, rows], st.at[:, 0, rows], 0, g_up),
        halo_copy(st.at[:, 1, rows], st.at[:, CX + 1, rows], 1, g_down),
        halo_copy(ys_hi, yr_lo, 2, s_up),
        halo_copy(ys_lo, yr_hi, 3, s_down),
    ]
    for copy in halo_copies:
        copy.start()

    for copy in ag1_copies:
        copy.wait_recv()
    line = ag1_src[...]
    for d in range(1, LINE):
        line = line + ag1[d]
    ag2_src[...] = line
    ag2_copies = [tile_copy(ag2_src, ag2.at[z], 1, d, z_peer(d)) for d in range(1, LINE)]
    for copy in ag2_copies:
        copy.start()
    ag2[z] = line

    def fugacity(x, _):
        e1, e2, e3 = e1_v[x], e2_v[x], e3_v[x]
        for i in range(NC):
            v = cb_t[i]
            cb = jnp.concatenate([v, v], axis=0)
            lnphi_ref[i, x] = (cb * e1 - e2 - um_v[i, x] * e3).astype(BF16)
        return 0

    lax.fori_loop(0, CX, fugacity, 0)

    for copy in rs1_copies:
        copy.wait_recv()
    part = rs1_src[z]
    for d in range(1, LINE):
        part = part + rs1[d]
    rs2_src[...] = part
    rs2_copies = [tile_copy(rs2_src, rs2.at[d], 3, d, y_peer(d)) for d in range(1, LINE)]
    for copy in rs2_copies:
        copy.start()

    for d in range(1, LINE):
        tile_copy(ag2_src, ag2.at[(z + LINE - d) % LINE], 1, d, z_peer(d)).wait_recv()
    table = ag2[...].reshape(LINE * LINE, LANES)
    p_seg = pick_rows(table, seg_hot, slot_hot > 0.5, 3)
    push = strength * (p_cell - p_seg)
    push_up, push_down = jnp.maximum(push, 0.0), jnp.minimum(push, 0.0)
    spread = jnp.concatenate([lane_hot * push_up, lane_hot * push_down], axis=0)
    dense = None
    for part in pieces_of(spread, 3):
        found = mm_nt(row_hot_b, part)
        dense = found if dense is None else dense + found
    wp_v[...] = dense[:, :LANES].reshape(CX, CY, LANES)
    wn_v[...] = dense[:, LANES:].reshape(CX, CY, LANES)

    for copy in halo_copies:
        copy.wait_recv()

    def put_rows(c, _):
        st[c, inner, 7, :] = yr_lo[c]
        st[c, inner, 8 + CY, :] = yr_hi[c]
        return 0

    lax.fori_loop(0, NC + 2, put_rows, 0)
    loads[7].wait()

    plane = (CY, LANES)
    y_id, lane_id = iota(plane, 0), iota(plane, 1)
    has_low = jnp.logical_or(y_id > 0, s > 0)
    has_high = jnp.logical_or(y_id < CY - 1, s < n_sub - 1)

    def flux(x, _):
        xc = x + 1
        p, k = st[NC, xc, rows, :], st[NC + 1, xc, rows, :]

        def side(p_b, k_b, factor):
            trans_ab = factor * 2.0 * k * k_b / (k + k_b)
            flow = trans_ab * (p - p_b)
            return jnp.maximum(flow, 0.0), jnp.minimum(flow, 0.0)

        f_low = jnp.where(jnp.logical_or(x > 0, g > 0), trans[0], 0.0)
        f_high = jnp.where(jnp.logical_or(x < CX - 1, g < n_grp - 1), trans[0], 0.0)
        up_rows, down_rows = pl.ds(9, CY), pl.ds(7, CY)
        faces = [
            side(st[NC, xc - 1, rows, :], st[NC + 1, xc - 1, rows, :], f_low),
            side(st[NC, xc + 1, rows, :], st[NC + 1, xc + 1, rows, :], f_high),
            side(
                st[NC, xc, down_rows, :],
                st[NC + 1, xc, down_rows, :],
                jnp.where(has_low, trans[1], 0.0),
            ),
            side(
                st[NC, xc, up_rows, :],
                st[NC + 1, xc, up_rows, :],
                jnp.where(has_high, trans[1], 0.0),
            ),
            side(
                pltpu.roll(p, 1, 1),
                pltpu.roll(k, 1, 1),
                jnp.where(lane_id > 0, trans[2], 0.0),
            ),
            side(
                pltpu.roll(p, LANES - 1, 1),
                pltpu.roll(k, LANES - 1, 1),
                jnp.where(lane_id < LANES - 1, trans[2], 0.0),
            ),
        ]
        diag = pv_v[x] + wp_v[x]
        for out, _in in faces:
            diag = diag + out
        gain = mob_v[x] * wn_v[x]
        coming = [f[1] for f in faces]
        for i in range(NC):
            v = inj_t[i]
            inj = jnp.concatenate([v, v], axis=0)
            c = st[i, xc, rows, :]
            r = c * diag + gain * inj - old_v[i, x]
            r = r + coming[0] * st[i, xc - 1, rows, :]
            r = r + coming[1] * st[i, xc + 1, rows, :]
            r = r + coming[2] * st[i, xc, down_rows, :]
            r = r + coming[3] * st[i, xc, up_rows, :]
            r = r + coming[4] * pltpu.roll(c, 1, 1)
            r = r + coming[5] * pltpu.roll(c, LANES - 1, 1)
            resid_ref[i, x] = r
        return 0

    lax.fori_loop(0, CX, flux, 0)

    for copy in rs2_copies:
        copy.wait_recv()
    full = rs2_src[...]
    for d in range(1, LINE):
        full = full + rs2[d]
    mine = jnp.sum(jnp.where(iota(tile, 0) == y, full, 0.0), axis=0, keepdims=True)
    mine = jnp.broadcast_to(mine, tile)
    row_v[...] = mine
    s0 = row_v[:, 0:32]
    s1 = row_v[:, 32:64]
    rate = s1 - (cpp - 1.0) * s0
    running = mm_full(rate, before_hot)
    well = base - friction[0] * running * jnp.abs(running)
    well_ref[...] = well[0:1]

    for copy in ag1_copies + ag2_copies + rs1_copies + rs2_copies + halo_copies:
        copy.wait_send()


def per_device(n_grp, n_sub, *args):
    (
        amounts,
        pressure,
        heat,
        flag,
        perm,
        pore,
        former,
        trans,
        visc,
        crit,
        attract,
        covol,
        kappa,
        kij,
        recipe,
        locale,
        member,
        piece,
        strength,
        place,
        order,
        seg_pressure,
        exit_pressure,
        friction,
    ) = args
    field = (CX, CY, LANES)
    every = (NC, CX, CY, LANES)
    hbm = pl.BlockSpec(memory_space=pltpu.HBM)
    smem = pl.BlockSpec(memory_space=pltpu.SMEM)
    vmem = pl.BlockSpec(memory_space=pltpu.VMEM)
    tiles = pltpu.VMEM((LINE, 8, LANES), F32)
    one = pltpu.VMEM((8, LANES), F32)
    table = pltpu.VMEM((NC, 8, LANES), F32)
    edge = pltpu.VMEM((NC + 2, CX, LANES), F32)
    scratch = [
        pltpu.VMEM(every, F32),
        pltpu.VMEM(field, F32),
        pltpu.VMEM(field, jnp.int32),
        pltpu.VMEM(field, F32),
        pltpu.VMEM(every, F32),
        pltpu.VMEM((NC + 2, CX + 2, CY + 16, LANES), F32),
        pltpu.VMEM(every, F32),
        pltpu.VMEM((NC, CX // 2, CY, LANES), F32),
        *[pltpu.VMEM(field, F32) for _ in range(7)],
        table,
        table,
        table,
        table,
        one,
        one,
        tiles,
        one,
        tiles,
        tiles,
        tiles,
        one,
        tiles,
        edge,
        edge,
        edge,
        edge,
        pltpu.SemaphoreType.DMA((8,)),
        pltpu.SemaphoreType.DMA((4, LINE)),
        pltpu.SemaphoreType.DMA((4, LINE)),
        pltpu.SemaphoreType.DMA((4,)),
        pltpu.SemaphoreType.DMA((4,)),
        pltpu.SemaphoreType.DMA((SMALL,)),
    ]
    small = (
        trans,
        visc,
        crit,
        attract,
        covol,
        kappa,
        kij,
        recipe,
        locale.reshape(2, LANES),
        member.reshape(2, LANES),
        piece.reshape(2, LANES),
        strength.reshape(2, LANES),
        place,
        order,
        seg_pressure,
    )
    spaces = [pltpu.SMEM] * SCALARS + [pltpu.VMEM] * (SMALL - SCALARS)
    held = [space(v.shape, v.dtype) for space, v in zip(spaces, small)]
    return pl.pallas_call(
        functools.partial(body, n_grp, n_sub),
        out_shape=(
            jax.ShapeDtypeStruct(every, F32),
            jax.ShapeDtypeStruct(every, BF16),
            jax.ShapeDtypeStruct((1, 32), F32),
        ),
        in_specs=[hbm] * (7 + SMALL) + [smem] * 2,
        out_specs=(vmem, vmem, vmem),
        scratch_shapes=held + scratch,
        compiler_params=pltpu.CompilerParams(
            collective_id=0, has_side_effects=True, vmem_limit_bytes=40 * 1024 * 1024
        ),
        name="newton_residual",
    )(
        *[
            pltpu.with_memory_space_constraint(v, pltpu.HBM)
            for v in (amounts, pressure, heat, flag, perm, pore, former, *small)
        ],
        exit_pressure,
        friction,
    )


def solution(mesh):
    areal = P("grp", "sub", None)
    every = P(None, "grp", "sub", None)
    both = P(("grp", "sub"))
    rows = P(("grp", "sub"), None)
    in_specs = (
        every,
        areal,
        areal,
        areal,
        areal,
        areal,
        every,
        *[P()] * 8,
        both,
        rows,
        both,
        both,
        P("grp", None),
        rows,
        rows,
        both,
        both,
    )
    return jax.shard_map(
        functools.partial(per_device, mesh.shape["grp"], mesh.shape["sub"]),
        mesh=mesh,
        in_specs=in_specs,
        out_specs=(every, every, rows),
        check_vma=False,
    )
```

```python
import functools
import math

import jax
import jax.numpy as jnp
from jax import lax
from jax.experimental import pallas as pl
from jax.experimental.pallas import tpu as pltpu
from jax.sharding import PartitionSpec as P

NEWT = 8
ROOT_TWO = math.sqrt(2.0)
MESH = pl.DeviceIdType.MESH
NC = 16
CX = 8
CY = 16
LANES = 128
LINE = 8
SMALL = 15
SCALARS = 8
F32 = jnp.float32
BF16 = jnp.bfloat16
HIGHEST = lax.Precision.HIGHEST


def away(step):
    return sum(min(d, LINE - d) for d in step)


STEPS = [(dz, dy) for dz in range(LINE) for dy in range(LINE) if dz or dy]
STEPS.sort(key=away, reverse=True)


def iota(shape, axis):
    return lax.broadcasted_iota(jnp.int32, shape, axis)


def hot(index_row, rows):
    mask = iota((rows, index_row.shape[1]), 0) == index_row
    return jnp.where(mask, 1.0, 0.0).astype(F32)


def pieces_of(x, count):
    out = []
    for _ in range(count):
        top = x.astype(BF16)
        out.append(top)
        x = x - top.astype(F32)
    return out


def mm(a, b):
    return lax.dot_general(a, b, (((1,), (0,)), ((), ())), preferred_element_type=F32)


def mm_nt(a, b):
    return lax.dot_general(a, b, (((1,), (1,)), ((), ())), preferred_element_type=F32)


def mm_full(a, b):
    return lax.dot_general(
        a, b, (((1,), (0,)), ((), ())), precision=HIGHEST, preferred_element_type=F32
    )


def mm_full_nt(a, b):
    return lax.dot_general(
        a, b, (((1,), (1,)), ((), ())), precision=HIGHEST, preferred_element_type=F32
    )


def pick_rows(field, lane_hot, row_mask, count):
    parts = pieces_of(field, count)
    found = mm(jnp.concatenate(parts, axis=0), lane_hot)
    rows = field.shape[0]
    total = found[:rows]
    for i in range(1, count):
        total = total + found[i * rows : (i + 1) * rows]
    return jnp.sum(jnp.where(row_mask, total, 0.0), axis=0, keepdims=True)


def body(
    n_grp,
    n_sub,
    n_hbm,
    p_hbm,
    t_hbm,
    flag_hbm,
    k_hbm,
    pore_hbm,
    old_hbm,
    *refs,
):
    small_hbm, refs = refs[:SMALL], refs[SMALL:]
    exit_p, friction, *refs = refs
    resid_ref, lnphi_ref, well_ref = refs[:3]
    small_refs, refs = refs[3 : 3 + SMALL], refs[3 + SMALL :]
    (
        trans,
        visc,
        crit,
        attract,
        covol,
        kappa,
        kij,
        recipe,
        loc_ref,
        mem_ref,
        seg_ref,
        wi_ref,
        gmp_ref,
        order_ref,
        cpp_ref,
    ) = small_refs
    (
        n_v,
        t_v,
        flag_v,
        pore_v,
        old_v,
        st,
        um_v,
        w_v,
        mob_v,
        e1_v,
        e2_v,
        e3_v,
        pv_v,
        wp_v,
        wn_v,
        c0_t,
        c1_t,
        cb_t,
        inj_t,
        row_v,
        mail_out,
        mail_in,
        ys_lo,
        ys_hi,
        yr_lo,
        yr_hi,
        in_sem,
        mail_send,
        mail_recv,
        halo_send,
        halo_recv,
        small_sem,
    ) = refs
    g = lax.axis_index("grp")
    s = lax.axis_index("sub")
    z, y = s // LINE, s % LINE

    def peer_at(dz, dy):
        return ((z + dz) % LINE) * LINE + (y + dy) % LINE

    mates = [peer_at(dz, dy) for dz, dy in STEPS]
    g_up, g_down = {"grp": (g + 1) % n_grp}, {"grp": (g + n_grp - 1) % n_grp}
    s_up, s_down = {"sub": (s + 1) % n_sub}, {"sub": (s + n_sub - 1) % n_sub}

    inner = pl.ds(1, CX)
    rows = pl.ds(8, CY)
    half = CX // 2
    loads = [
        pltpu.make_async_copy(t_hbm, t_v, in_sem.at[0]),
        pltpu.make_async_copy(p_hbm, st.at[NC, inner, rows], in_sem.at[1]),
        pltpu.make_async_copy(n_hbm.at[:, pl.ds(0, half)], n_v.at[:, pl.ds(0, half)], in_sem.at[2]),
        pltpu.make_async_copy(
            n_hbm.at[:, pl.ds(half, half)], n_v.at[:, pl.ds(half, half)], in_sem.at[3]
        ),
        pltpu.make_async_copy(flag_hbm, flag_v, in_sem.at[4]),
        pltpu.make_async_copy(k_hbm, st.at[NC + 1, inner, rows], in_sem.at[5]),
        pltpu.make_async_copy(pore_hbm, pore_v, in_sem.at[6]),
        pltpu.make_async_copy(old_hbm, old_v, in_sem.at[7]),
    ]
    small_loads = [
        pltpu.make_async_copy(src, dst, small_sem.at[i])
        for i, (src, dst) in enumerate(zip(small_hbm, small_refs))
    ]
    for load in small_loads[SCALARS:] + loads[:3]:
        load.start()
    for load in small_loads[:SCALARS]:
        load.start()

    barrier = pltpu.get_barrier_semaphore()
    peers = [{"sub": mate} for mate in mates] + [g_up, g_down]
    for peer in peers:
        pl.semaphore_signal(barrier, inc=1, device_id=peer, device_id_type=MESH)
    for load in loads[3:]:
        load.start()

    for load in small_loads:
        load.wait()

    tile = (8, LANES)
    total = jnp.zeros(tile, F32)
    for i in range(NC):
        total = total + recipe[i]
    for i in range(NC):
        amount = jnp.sqrt(jnp.full(tile, attract[i], F32))
        slope = jnp.full(tile, kappa[i], F32)
        c0_t[i] = amount * (1.0 + slope)
        c1_t[i] = amount * slope / jnp.sqrt(jnp.full(tile, crit[i], F32))
        cb_t[i] = jnp.full(tile, covol[i], F32)
        inj_t[i] = jnp.full(tile, recipe[i], F32) / total

    row_v[...] = jnp.zeros(tile, F32)
    row_v[0:1, 64:96] = cpp_ref[...]
    own_row = row_v[0:1, :]

    loc = [loc_ref[h : h + 1, :] for h in range(2)]
    row_of = jnp.concatenate([v // LANES for v in loc], axis=1)
    lane_of = jnp.concatenate([v % LANES for v in loc], axis=1)
    member = jnp.concatenate([mem_ref[h : h + 1, :] for h in range(2)], axis=1)
    segment = jnp.concatenate([seg_ref[h : h + 1, :] for h in range(2)], axis=1)
    strength = jnp.concatenate([wi_ref[h : h + 1, :] for h in range(2)], axis=1)
    wells = n_sub
    place = jnp.where(iota((wells, wells), 0) == gmp_ref[...], 1.0, 0.0).astype(BF16)
    slot_hot = mm(place, hot(member, wells).astype(BF16))
    lane_hot = hot(lane_of, LANES)
    lane_hot_b = lane_hot.astype(BF16)
    row_mask = iota((LANES, 2 * LANES), 0) == row_of
    row_hot_b = jnp.where(row_mask, 1.0, 0.0).astype(BF16)
    seg_hot = hot(segment, LANES).astype(BF16)
    seg_hot_2 = hot(segment + 32, LANES).astype(BF16)
    seg_hot_3 = hot(segment + 64, LANES).astype(BF16)

    order = jnp.where(iota((32, 32), 0) == order_ref[...], 1.0, 0.0).astype(F32)
    sub32, lane32 = iota((32, 32), 0), iota((32, 32), 1)
    upper = jnp.where(sub32 <= lane32, 1.0, 0.0).astype(F32)
    after = jnp.where(sub32 == lane32 + 1, 1.0, 0.0).astype(F32)
    before_hot = mm_full_nt(mm_full(order, upper), order)
    next_hot = mm_full_nt(mm_full(order, after), order)
    last_row = jnp.where(iota((8, 32), 1) == 31, 1.0, 0.0).astype(F32)
    last_hot = mm_full_nt(last_row, order)
    cpp = jnp.broadcast_to(cpp_ref[...], (8, 32))
    base = cpp - (mm_full(cpp, next_hot) + exit_p[0] * last_hot)

    loads[0].wait()
    loads[1].wait()
    loads[4].wait()
    loads[6].wait()

    def phase(b, _):
        xs = pl.ds(b * half, half)
        xp = pl.ds(b * half + 1, half)
        pltpu.make_async_copy(n_hbm.at[:, xs], n_v.at[:, xs], in_sem.at[2 + b]).wait()
        t = t_v[xs]
        p = st[NC, xp, rows, :]
        root_t = jnp.sqrt(t)
        whole = jnp.zeros_like(t)
        bsum = jnp.zeros_like(t)

        def wide(table, i):
            v = table[i]
            return jnp.broadcast_to(
                jnp.concatenate([v, v], axis=0)[None], (half, CY, LANES)
            )

        for i in range(NC):
            n = n_v[i, xs]
            u = jnp.abs(wide(c0_t, i) - wide(c1_t, i) * root_t)
            um_v[i, xs] = u
            w_v[i] = n * u
            whole = whole + n
            bsum = bsum + wide(cb_t, i) * n
        asum = jnp.zeros_like(t)
        for i in range(NC):
            m = None
            for j in range(NC):
                term = w_v[j] * (1.0 - kij[i, j])
                m = term if m is None else m + term
            um = um_v[i, xs] * m
            um_v[i, xs] = um
            asum = asum + n_v[i, xs] * um
        inv = 1.0 / whole
        inv_t = 1.0 / t
        pt = p * inv_t
        gain = pt * inv_t * inv
        big_a = gain * inv * asum
        big_b = pt * inv * bsum
        liquid = flag_v[xs] == 1
        zed = jnp.where(liquid, big_b + 0.01, 1.0 + big_b)
        low = big_b + 0.01
        c2 = big_b - 1.0
        c2x2 = 2.0 * c2
        c1 = big_a - 3.0 * big_b * big_b - 2.0 * big_b
        c0 = big_b * big_b + big_b * big_b * big_b - big_a * big_b
        for _step in range(NEWT):
            value = ((zed + c2) * zed + c1) * zed + c0
            slope = (3.0 * zed + c2x2) * zed + c1
            zed = jnp.maximum(zed - value / jnp.maximum(slope, 0.1), low)
        ratio = jnp.log((zed + (1.0 + ROOT_TWO) * big_b) / (zed + (1.0 - ROOT_TWO) * big_b))
        inv_b = 1.0 / big_b
        e3 = ratio * inv_b * (1.0 / ROOT_TWO)
        e1_v[xs] = pt * inv_b * ((zed - 1.0) + 0.5 * big_a * e3)
        e2_v[xs] = jnp.log(zed - big_b)
        e3_v[xs] = e3 * gain
        thick = jnp.where(liquid, visc[1], visc[0])
        mob = pt / (zed * thick)
        mob_v[xs] = mob
        pv_v[xs] = pore_v[xs] * thick
        share = mob * inv
        for i in range(NC):
            st[i, xp, rows, :] = n_v[i, xs] * share
        return 0

    lax.fori_loop(0, 2, phase, 0)

    p_cell = pick_rows(
        st[NC, inner, rows, :].reshape(LANES, LANES), lane_hot_b, row_mask, 3
    )
    mob_cell = pick_rows(mob_v[...].reshape(LANES, LANES), lane_hot_b, row_mask, 2)
    v0 = strength * mob_cell
    v1 = v0 * (p_cell - 1.0)
    left = jnp.concatenate([slot_hot * v0, slot_hot * v1], axis=1)
    right = jnp.concatenate([seg_hot, seg_hot_2], axis=1)
    sums = None
    for part in pieces_of(left, 3):
        found = mm_nt(part, right)
        sums = found if sums is None else sums + found
    mail_out[...] = (sums + own_row).reshape(n_sub, 1, LANES)
    mail_in[s] = mail_out[s]

    pl.semaphore_wait(barrier, len(peers))
    for mate in mates:
        pltpu.make_async_remote_copy(
            src_ref=mail_out.at[mate],
            dst_ref=mail_in.at[s],
            send_sem=mail_send,
            recv_sem=mail_recv,
            device_id={"sub": mate},
            device_id_type=MESH,
        ).start()
    mail = pltpu.make_async_remote_copy(
        src_ref=mail_out.at[pl.ds(0, n_sub - 1)],
        dst_ref=mail_in.at[pl.ds(0, n_sub - 1)],
        send_sem=mail_send,
        recv_sem=mail_recv,
        device_id=g_up,
        device_id_type=MESH,
    )

    loads[5].wait()

    def gather_rows(c, _):
        ys_lo[c] = st[c, inner, 8, :]
        ys_hi[c] = st[c, inner, 8 + CY - 1, :]
        return 0

    lax.fori_loop(0, NC + 2, gather_rows, 0)

    def halo_copy(src, dst, slot, peer):
        return pltpu.make_async_remote_copy(
            src_ref=src,
            dst_ref=dst,
            send_sem=halo_send.at[slot],
            recv_sem=halo_recv.at[slot],
            device_id=peer,
            device_id_type=MESH,
        )

    halo_copies = [
        halo_copy(st.at[:, CX, rows], st.at[:, 0, rows], 0, g_up),
        halo_copy(st.at[:, 1, rows], st.at[:, CX + 1, rows], 1, g_down),
        halo_copy(ys_hi, yr_lo, 2, s_up),
        halo_copy(ys_lo, yr_hi, 3, s_down),
    ]
    for copy in halo_copies:
        copy.start()

    def fugacity(x, _):
        e1, e2, e3 = e1_v[x], e2_v[x], e3_v[x]
        for i in range(NC):
            v = cb_t[i]
            cb = jnp.concatenate([v, v], axis=0)
            lnphi_ref[i, x] = (cb * e1 - e2 - um_v[i, x] * e3).astype(BF16)
        return 0

    lax.fori_loop(0, CX, fugacity, 0)

    for copy in halo_copies:
        copy.wait_recv()

    def put_rows(c, _):
        st[c, inner, 7, :] = yr_lo[c]
        st[c, inner, 8 + CY, :] = yr_hi[c]
        return 0

    lax.fori_loop(0, NC + 2, put_rows, 0)
    loads[7].wait()

    plane = (CY, LANES)
    y_id, lane_id = iota(plane, 0), iota(plane, 1)
    has_low = jnp.logical_or(y_id > 0, s > 0)
    has_high = jnp.logical_or(y_id < CY - 1, s < n_sub - 1)

    def flux(x, _):
        xc = x + 1
        p, k = st[NC, xc, rows, :], st[NC + 1, xc, rows, :]

        def side(p_b, k_b, factor):
            trans_ab = factor * 2.0 * k * k_b / (k + k_b)
            flow = trans_ab * (p - p_b)
            return jnp.maximum(flow, 0.0), jnp.minimum(flow, 0.0)

        f_low = jnp.where(jnp.logical_or(x > 0, g > 0), trans[0], 0.0)
        f_high = jnp.where(jnp.logical_or(x < CX - 1, g < n_grp - 1), trans[0], 0.0)
        up_rows, down_rows = pl.ds(9, CY), pl.ds(7, CY)
        faces = [
            side(st[NC, xc - 1, rows, :], st[NC + 1, xc - 1, rows, :], f_low),
            side(st[NC, xc + 1, rows, :], st[NC + 1, xc + 1, rows, :], f_high),
            side(
                st[NC, xc, down_rows, :],
                st[NC + 1, xc, down_rows, :],
                jnp.where(has_low, trans[1], 0.0),
            ),
            side(
                st[NC, xc, up_rows, :],
                st[NC + 1, xc, up_rows, :],
                jnp.where(has_high, trans[1], 0.0),
            ),
            side(
                pltpu.roll(p, 1, 1),
                pltpu.roll(k, 1, 1),
                jnp.where(lane_id > 0, trans[2], 0.0),
            ),
            side(
                pltpu.roll(p, LANES - 1, 1),
                pltpu.roll(k, LANES - 1, 1),
                jnp.where(lane_id < LANES - 1, trans[2], 0.0),
            ),
        ]
        diag = pv_v[x]
        for out, _in in faces:
            diag = diag + out
        coming = [f[1] for f in faces]
        for i in range(NC):
            c = st[i, xc, rows, :]
            r = c * diag - old_v[i, x]
            r = r + coming[0] * st[i, xc - 1, rows, :]
            r = r + coming[1] * st[i, xc + 1, rows, :]
            r = r + coming[2] * st[i, xc, down_rows, :]
            r = r + coming[3] * st[i, xc, up_rows, :]
            r = r + coming[4] * pltpu.roll(c, 1, 1)
            r = r + coming[5] * pltpu.roll(c, LANES - 1, 1)
            resid_ref[i, x] = r
        return 0

    lax.fori_loop(0, CX, flux, 0)

    for copy in halo_copies:
        copy.wait_send()
    mail.wait_send()

    mail.wait_recv()
    table = mail_in[...].reshape(n_sub, LANES)
    p_seg = pick_rows(table, seg_hot_3, slot_hot > 0.5, 3)
    push = strength * (p_cell - p_seg)
    push_up, push_down = jnp.maximum(push, 0.0), jnp.minimum(push, 0.0)
    spread = jnp.concatenate([lane_hot * push_up, lane_hot * push_down], axis=0)
    dense = None
    for part in pieces_of(spread, 2):
        found = mm_nt(row_hot_b, part)
        dense = found if dense is None else dense + found
    wp_v[...] = dense[:, :LANES].reshape(CX, CY, LANES)
    wn_v[...] = dense[:, LANES:].reshape(CX, CY, LANES)

    mine = jnp.sum(table, axis=0, keepdims=True)
    row_v[...] = jnp.broadcast_to(mine, tile)
    rate = row_v[:, 32:64] - (cpp - 1.0) * row_v[:, 0:32]
    running = mm_full(rate, before_hot)
    well = base - friction[0] * running * jnp.abs(running)
    well_ref[...] = well[0:1]

    def perforated(x, _):
        wp, gain = wp_v[x], mob_v[x] * wn_v[x]
        for i in range(NC):
            v = inj_t[i]
            inj = jnp.concatenate([v, v], axis=0)
            resid_ref[i, x] = resid_ref[i, x] + (st[i, x + 1, rows, :] * wp + gain * inj)
        return 0

    lax.fori_loop(0, CX, perforated, 0)


def put(resid, lnphi, well, resid_out, lnphi_out, well_out, sem):
    pairs = ((resid, resid_out), (lnphi, lnphi_out), (well, well_out))
    copies = [pltpu.make_async_copy(a, b, sem.at[i]) for i, (a, b) in enumerate(pairs)]
    for copy in copies:
        copy.start()
    for copy in copies:
        copy.wait()


def per_device(n_grp, n_sub, *args):
    (
        amounts,
        pressure,
        heat,
        flag,
        perm,
        pore,
        former,
        trans,
        visc,
        crit,
        attract,
        covol,
        kappa,
        kij,
        recipe,
        locale,
        member,
        piece,
        strength,
        place,
        order,
        seg_pressure,
        exit_pressure,
        friction,
    ) = args
    field = (CX, CY, LANES)
    every = (NC, CX, CY, LANES)
    hbm = pl.BlockSpec(memory_space=pltpu.HBM)
    smem = pl.BlockSpec(memory_space=pltpu.SMEM)
    vmem = pl.BlockSpec(memory_space=pltpu.VMEM)
    mail = pltpu.VMEM((n_sub, 1, LANES), F32)
    one = pltpu.VMEM((8, LANES), F32)
    table = pltpu.VMEM((NC, 8, LANES), F32)
    edge = pltpu.VMEM((NC + 2, CX, LANES), F32)
    scratch = [
        pltpu.VMEM(every, F32),
        pltpu.VMEM(field, F32),
        pltpu.VMEM(field, jnp.int32),
        pltpu.VMEM(field, F32),
        pltpu.VMEM(every, F32),
        pltpu.VMEM((NC + 2, CX + 2, CY + 16, LANES), F32),
        pltpu.VMEM(every, F32),
        pltpu.VMEM((NC, CX // 2, CY, LANES), F32),
        *[pltpu.VMEM(field, F32) for _ in range(7)],
        table,
        table,
        table,
        table,
        one,
        mail,
        mail,
        edge,
        edge,
        edge,
        edge,
        pltpu.SemaphoreType.DMA((8,)),
        pltpu.SemaphoreType.DMA,
        pltpu.SemaphoreType.DMA,
        pltpu.SemaphoreType.DMA((4,)),
        pltpu.SemaphoreType.DMA((4,)),
        pltpu.SemaphoreType.DMA((SMALL,)),
    ]
    small = (
        trans,
        visc,
        crit,
        attract,
        covol,
        kappa,
        kij,
        recipe,
        locale.reshape(2, LANES),
        member.reshape(2, LANES),
        piece.reshape(2, LANES),
        strength.reshape(2, LANES),
        place,
        order,
        seg_pressure,
    )
    spaces = [pltpu.SMEM] * SCALARS + [pltpu.VMEM] * (SMALL - SCALARS)
    held = [space(v.shape, v.dtype) for space, v in zip(spaces, small)]
    outs = (
        jax.ShapeDtypeStruct(every, F32),
        jax.ShapeDtypeStruct(every, BF16),
        jax.ShapeDtypeStruct((1, 32), F32),
    )
    found = pl.pallas_call(
        functools.partial(body, n_grp, n_sub),
        out_shape=outs,
        in_specs=[hbm] * (7 + SMALL) + [smem] * 2,
        out_specs=(vmem, vmem, vmem),
        scratch_shapes=held + scratch,
        compiler_params=pltpu.CompilerParams(
            collective_id=0, has_side_effects=True, vmem_limit_bytes=40 * 1024 * 1024
        ),
        name="newton_residual",
    )(
        *[
            pltpu.with_memory_space_constraint(v, pltpu.HBM)
            for v in (amounts, pressure, heat, flag, perm, pore, former, *small)
        ],
        exit_pressure,
        friction,
    )
    return pl.pallas_call(
        put,
        out_shape=outs,
        in_specs=[vmem] * 3,
        out_specs=(hbm,) * 3,
        scratch_shapes=[pltpu.SemaphoreType.DMA((3,))],
        compiler_params=pltpu.CompilerParams(vmem_limit_bytes=4 * 1024 * 1024),
        name="put_outputs",
    )(*found)


def solution(mesh):
    areal = P("grp", "sub", None)
    every = P(None, "grp", "sub", None)
    both = P(("grp", "sub"))
    rows = P(("grp", "sub"), None)
    in_specs = (
        every,
        areal,
        areal,
        areal,
        areal,
        areal,
        every,
        *[P()] * 8,
        both,
        rows,
        both,
        both,
        P("grp", None),
        rows,
        rows,
        both,
        both,
    )
    return jax.shard_map(
        functools.partial(per_device, mesh.shape["grp"], mesh.shape["sub"]),
        mesh=mesh,
        in_specs=in_specs,
        out_specs=(every, every, rows),
        check_vma=False,
    )
```

```python
import functools
import math

import jax
import jax.numpy as jnp
from jax import lax
from jax.experimental import pallas as pl
from jax.experimental.pallas import tpu as pltpu
from jax.sharding import PartitionSpec as P

NEWT = 8
ROOT_TWO = math.sqrt(2.0)
MESH = pl.DeviceIdType.MESH
NC = 16
CX = 8
CY = 16
LANES = 128
LINE = 8
SMALL = 15
SCALARS = 8
F32 = jnp.float32
BF16 = jnp.bfloat16
HIGHEST = lax.Precision.HIGHEST


def iota(shape, axis):
    return lax.broadcasted_iota(jnp.int32, shape, axis)


def hot(index_row, rows):
    mask = iota((rows, index_row.shape[1]), 0) == index_row
    return jnp.where(mask, 1.0, 0.0).astype(F32)


def pieces_of(x, count):
    out = []
    for _ in range(count):
        top = x.astype(BF16)
        out.append(top)
        x = x - top.astype(F32)
    return out


def mm(a, b):
    return lax.dot_general(a, b, (((1,), (0,)), ((), ())), preferred_element_type=F32)


def mm_nt(a, b):
    return lax.dot_general(a, b, (((1,), (1,)), ((), ())), preferred_element_type=F32)


def mm_full(a, b):
    return lax.dot_general(
        a, b, (((1,), (0,)), ((), ())), precision=HIGHEST, preferred_element_type=F32
    )


def mm_full_nt(a, b):
    return lax.dot_general(
        a, b, (((1,), (1,)), ((), ())), precision=HIGHEST, preferred_element_type=F32
    )


def pick_rows(field, lane_hot, row_mask, count):
    parts = pieces_of(field, count)
    found = mm(jnp.concatenate(parts, axis=0), lane_hot)
    rows = field.shape[0]
    total = found[:rows]
    for i in range(1, count):
        total = total + found[i * rows : (i + 1) * rows]
    return jnp.sum(jnp.where(row_mask, total, 0.0), axis=0, keepdims=True)


def body(
    n_grp,
    n_sub,
    n_hbm,
    p_hbm,
    t_hbm,
    flag_hbm,
    k_hbm,
    pore_hbm,
    old_hbm,
    *refs,
):
    small_hbm, refs = refs[:SMALL], refs[SMALL:]
    exit_p, friction, *refs = refs
    resid_ref, lnphi_ref, well_ref = refs[:3]
    small_refs, refs = refs[3 : 3 + SMALL], refs[3 + SMALL :]
    (
        trans,
        visc,
        crit,
        attract,
        covol,
        kappa,
        kij,
        recipe,
        loc_ref,
        mem_ref,
        seg_ref,
        wi_ref,
        gmp_ref,
        order_ref,
        cpp_ref,
    ) = small_refs
    (
        n_v,
        t_v,
        flag_v,
        pore_v,
        old_v,
        st,
        up_v,
        w_v,
        mob_v,
        e1_v,
        e2_v,
        e3_v,
        root_v,
        inv_v,
        pt_v,
        gain_v,
        a_v,
        b_v,
        z_v,
        wp_v,
        wn_v,
        c0_t,
        c1_t,
        cb_t,
        inj_t,
        row_v,
        mail_out,
        mail_in,
        ys_lo,
        ys_hi,
        yr_lo,
        yr_hi,
        in_sem,
        mail_send,
        mail_recv,
        ready,
        halo_send,
        halo_recv,
        small_sem,
    ) = refs
    g = lax.axis_index("grp")
    s = lax.axis_index("sub")
    g_up, g_down = {"grp": (g + 1) % n_grp}, {"grp": (g + n_grp - 1) % n_grp}
    s_up, s_down = {"sub": (s + 1) % n_sub}, {"sub": (s + n_sub - 1) % n_sub}
    line = s // LINE
    has_g_up, has_g_down = g < n_grp - 1, g > 0
    has_s_up, has_s_down = s < n_sub - 1, s > 0

    inner = pl.ds(1, CX)
    rows = pl.ds(8, CY)
    half = CX // 2
    loads = [
        pltpu.make_async_copy(t_hbm, t_v, in_sem.at[0]),
        pltpu.make_async_copy(p_hbm, st.at[NC, inner, rows], in_sem.at[1]),
        pltpu.make_async_copy(n_hbm.at[:, pl.ds(0, half)], n_v.at[:, pl.ds(0, half)], in_sem.at[2]),
        pltpu.make_async_copy(
            n_hbm.at[:, pl.ds(half, half)], n_v.at[:, pl.ds(half, half)], in_sem.at[3]
        ),
        pltpu.make_async_copy(flag_hbm, flag_v, in_sem.at[4]),
        pltpu.make_async_copy(k_hbm, st.at[NC + 1, inner, rows], in_sem.at[5]),
        pltpu.make_async_copy(pore_hbm, pore_v, in_sem.at[6]),
        pltpu.make_async_copy(old_hbm, old_v, in_sem.at[7]),
    ]
    small_loads = [
        pltpu.make_async_copy(src, dst, small_sem.at[i])
        for i, (src, dst) in enumerate(zip(small_hbm, small_refs))
    ]
    for load in small_loads + loads[:4]:
        load.start()

    barrier = pltpu.get_barrier_semaphore()

    def greet(there, peer):
        @pl.when(there)
        def _():
            pl.semaphore_signal(barrier, inc=1, device_id=peer, device_id_type=MESH)

    def greet_higher(j, _):
        pl.semaphore_signal(barrier, inc=1, device_id={"sub": j}, device_id_type=MESH)
        return 0

    greet(has_g_up, g_up)
    greet(has_g_down, g_down)
    greet(has_s_down, s_down)
    lax.fori_loop(s + 1, n_sub, greet_higher, 0)
    expected = (
        s
        + has_s_up.astype(jnp.int32)
        + has_g_up.astype(jnp.int32)
        + has_g_down.astype(jnp.int32)
    )
    for load in loads[4:]:
        load.start()

    for load in small_loads:
        load.wait()

    tile = (8, LANES)
    for i in range(NC):
        amount = jnp.sqrt(jnp.full(tile, attract[i], F32))
        slope = jnp.full(tile, kappa[i], F32)
        c0_t[i] = amount * (1.0 + slope)
        c1_t[i] = amount * slope / jnp.sqrt(jnp.full(tile, crit[i], F32))
        cb_t[i] = jnp.full(tile, covol[i], F32)

    row_v[...] = jnp.zeros(tile, F32)
    row_v[0:1, 64:96] = cpp_ref[...] - 1.0
    own_row = row_v[0:1, :]

    loc = [loc_ref[h : h + 1, :] for h in range(2)]
    row_of = jnp.concatenate([v // LANES for v in loc], axis=1)
    lane_of = jnp.concatenate([v % LANES for v in loc], axis=1)
    member = jnp.concatenate([mem_ref[h : h + 1, :] for h in range(2)], axis=1)
    segment = jnp.concatenate([seg_ref[h : h + 1, :] for h in range(2)], axis=1)
    strength = jnp.concatenate([wi_ref[h : h + 1, :] for h in range(2)], axis=1)
    wells = n_sub
    place = jnp.where(iota((wells, wells), 0) == gmp_ref[...], 1.0, 0.0).astype(BF16)
    slot_hot = mm(place, hot(member, wells).astype(BF16))
    lane_hot = hot(lane_of, LANES)
    lane_hot_b = lane_hot.astype(BF16)
    row_mask = iota((LANES, 2 * LANES), 0) == row_of
    row_hot_b = jnp.where(row_mask, 1.0, 0.0).astype(BF16)
    seg_hot = hot(segment, LANES).astype(BF16)
    seg_hot_2 = hot(segment + 32, LANES).astype(BF16)
    seg_hot_3 = hot(segment + 64, LANES).astype(BF16)

    def wide(table, i):
        v = table[i]
        return jnp.broadcast_to(jnp.concatenate([v, v], axis=0)[None], (half, CY, LANES))

    loads[0].wait()
    loads[1].wait()

    def phase(b, _):
        xs = pl.ds(b * half, half)
        xp = pl.ds(b * half + 1, half)
        pltpu.make_async_copy(n_hbm.at[:, xs], n_v.at[:, xs], in_sem.at[2 + b]).wait()
        t = t_v[xs]
        root_t = jnp.sqrt(t)
        root_v[xs] = root_t
        whole = jnp.zeros_like(t)
        bsum = jnp.zeros_like(t)
        for i in range(NC):
            n = n_v[i, xs]
            w_v[i, xs] = n * jnp.abs(wide(c0_t, i) - wide(c1_t, i) * root_t)
            whole = whole + n
            bsum = bsum + wide(cb_t, i) * n
        last = w_v[NC - 1, xs]
        asum = last * last
        for i in range(NC - 1):
            m = None
            for j in range(i + 1, NC):
                term = w_v[j, xs] * (1.0 - kij[i, j])
                m = term if m is None else m + term
            up_v[i, xs] = m
            w = w_v[i, xs]
            asum = asum + w * (w + 2.0 * m)
        inv = 1.0 / whole
        inv_t = 1.0 / t
        pt = st[NC, xp, rows, :] * inv_t
        gain = pt * inv_t * inv
        inv_v[xs] = inv
        pt_v[xs] = pt
        gain_v[xs] = gain
        a_v[xs] = gain * inv * asum
        b_v[xs] = pt * inv * bsum
        return 0

    lax.fori_loop(0, 2, phase, 0)

    loads[4].wait()
    big_a, big_b = a_v[...], b_v[...]
    liquid = flag_v[...] == 1
    zed = jnp.where(liquid, big_b + 0.01, 1.0 + big_b)
    c1 = big_a - 3.0 * big_b * big_b - 2.0 * big_b
    c0 = big_b * big_b + big_b * big_b * big_b - big_a * big_b
    for _step in range(NEWT):
        c2 = big_b - 1.0
        value = ((zed + c2) * zed + c1) * zed + c0
        slope = (3.0 * zed + 2.0 * c2) * zed + c1
        zed = jnp.maximum(zed - value / jnp.maximum(slope, 0.1), big_b + 0.01)
    z_v[...] = zed
    mob_v[...] = pt_v[...] / (zed * jnp.where(liquid, visc[1], visc[0]))

    p_cell = pick_rows(
        st[NC, inner, rows, :].reshape(LANES, LANES) - 1.0, lane_hot_b, row_mask, 2
    )
    mob_cell = pick_rows(mob_v[...].reshape(LANES, LANES), lane_hot_b, row_mask, 2)
    v0 = strength * mob_cell
    v1 = v0 * p_cell
    left = jnp.concatenate([slot_hot * v0, slot_hot * v1], axis=1)
    right = jnp.concatenate([seg_hot, seg_hot_2], axis=1)
    sums = None
    for part in pieces_of(left, 2):
        found = mm_nt(part, right)
        sums = found if sums is None else sums + found
    mail_out[...] = (sums + own_row).reshape(n_sub, 1, LANES)
    mail_in[s] = mail_out[s]

    def post(j, _):
        pltpu.make_async_remote_copy(
            src_ref=mail_out.at[j],
            dst_ref=mail_in.at[s],
            send_sem=mail_send,
            recv_sem=mail_recv,
            device_id={"sub": j},
            device_id_type=MESH,
        ).start()
        return 0

    def tell(j, _):
        pl.semaphore_signal(
            ready.at[line], inc=1, device_id={"sub": j}, device_id_type=MESH
        )
        return 0

    pl.semaphore_wait(barrier, expected)
    lax.fori_loop(0, s, post, 0)
    lax.fori_loop(0, s, tell, 0)
    mail = pltpu.make_async_remote_copy(
        src_ref=mail_out.at[pl.ds(0, n_sub - 1)],
        dst_ref=mail_in.at[pl.ds(0, n_sub - 1)],
        send_sem=mail_send,
        recv_sem=mail_recv,
        device_id=g_up,
        device_id_type=MESH,
    )

    def carry(x, _):
        share = mob_v[x] * inv_v[x]
        for i in range(NC):
            st[i, x + 1, rows, :] = n_v[i, x] * share
        return 0

    lax.fori_loop(0, CX, carry, 0)
    loads[5].wait()

    def gather_rows(c, _):
        ys_lo[c] = st[c, inner, 8, :]
        ys_hi[c] = st[c, inner, 8 + CY - 1, :]
        return 0

    lax.fori_loop(0, NC + 2, gather_rows, 0)

    def halo_copy(src, dst, slot, peer):
        return pltpu.make_async_remote_copy(
            src_ref=src,
            dst_ref=dst,
            send_sem=halo_send.at[slot],
            recv_sem=halo_recv.at[slot],
            device_id=peer,
            device_id_type=MESH,
        )

    halo_copies = [
        halo_copy(st.at[:, CX, rows], st.at[:, 0, rows], 0, g_up),
        halo_copy(st.at[:, 1, rows], st.at[:, CX + 1, rows], 1, g_down),
        halo_copy(ys_hi, yr_lo, 2, s_up),
        halo_copy(ys_lo, yr_hi, 3, s_down),
    ]
    sends = (has_g_up, has_g_down, has_s_up, has_s_down)
    receives = (has_g_down, has_g_up, has_s_down, has_s_up)

    for there, copy in zip(sends, halo_copies):
        pl.when(there)(copy.start)

    @pl.when(jnp.logical_not(has_g_down))
    def _():
        st[:, 0, rows, :] = jnp.zeros((NC + 2, CY, LANES), F32)

    @pl.when(jnp.logical_not(has_g_up))
    def _():
        st[:, CX + 1, rows, :] = jnp.zeros((NC + 2, CY, LANES), F32)

    @pl.when(jnp.logical_not(has_s_down))
    def _():
        yr_lo[...] = jnp.zeros((NC + 2, CX, LANES), F32)

    @pl.when(jnp.logical_not(has_s_up))
    def _():
        yr_hi[...] = jnp.zeros((NC + 2, CX, LANES), F32)

    total = jnp.zeros(tile, F32)
    for i in range(NC):
        total = total + recipe[i]
    for i in range(NC):
        inj_t[i] = jnp.full(tile, recipe[i], F32) / total

    order = jnp.where(iota((32, 32), 0) == order_ref[...], 1.0, 0.0).astype(F32)
    sub32, lane32 = iota((32, 32), 0), iota((32, 32), 1)
    upper = jnp.where(sub32 <= lane32, 1.0, 0.0).astype(F32)
    after = jnp.where(sub32 == lane32 + 1, 1.0, 0.0).astype(F32)
    before_hot = mm_full_nt(mm_full(order, upper), order)
    next_hot = mm_full_nt(mm_full(order, after), order)
    last_row = jnp.where(iota((8, 32), 1) == 31, 1.0, 0.0).astype(F32)
    last_hot = mm_full_nt(last_row, order)
    cpp = jnp.broadcast_to(cpp_ref[...], (8, 32))
    base = cpp - (mm_full(cpp, next_hot) + exit_p[0] * last_hot)


    loads[6].wait()

    def fugacity(b, _):
        xs = pl.ds(b * half, half)
        zed, big_b, pt = z_v[xs], b_v[xs], pt_v[xs]
        ratio = jnp.log((zed + (1.0 + ROOT_TWO) * big_b) / (zed + (1.0 - ROOT_TWO) * big_b))
        inv_b = 1.0 / big_b
        e3 = ratio * inv_b * (1.0 / ROOT_TWO)
        e1_v[xs] = pt * inv_b * ((zed - 1.0) + 0.5 * a_v[xs] * e3)
        e2_v[xs] = jnp.log(zed - big_b)
        e3_v[xs] = e3 * gain_v[xs]
        pore_v[xs] = pore_v[xs] * jnp.where(flag_v[xs] == 1, visc[1], visc[0])
        for i in range(NC):
            m = w_v[i, xs]
            if i < NC - 1:
                m = m + up_v[i, xs]
            for j in range(i):
                m = m + w_v[j, xs] * (1.0 - kij[i, j])
            u = jnp.abs(wide(c0_t, i) - wide(c1_t, i) * root_v[xs])
            part = wide(cb_t, i) * e1_v[xs] - e2_v[xs]
            lnphi_ref[i, xs] = (part - u * m * e3_v[xs]).astype(BF16)
        return 0

    lax.fori_loop(0, 2, fugacity, 0)

    for there, copy in zip(receives, halo_copies):
        pl.when(there)(copy.wait_recv)

    def put_rows(c, _):
        st[c, inner, 7, :] = yr_lo[c]
        st[c, inner, 8 + CY, :] = yr_hi[c]
        return 0

    lax.fori_loop(0, NC + 2, put_rows, 0)
    loads[7].wait()

    plane = (CY, LANES)
    lane_id = iota(plane, 1)

    def flux(x, _):
        xc = x + 1
        p, k = st[NC, xc, rows, :], st[NC + 1, xc, rows, :]

        def side(p_b, k_b, factor):
            trans_ab = factor * 2.0 * k * k_b / (k + k_b)
            flow = trans_ab * (p - p_b)
            return jnp.maximum(flow, 0.0), jnp.minimum(flow, 0.0)

        up_rows, down_rows = pl.ds(9, CY), pl.ds(7, CY)
        faces = [
            side(st[NC, xc - 1, rows, :], st[NC + 1, xc - 1, rows, :], trans[0]),
            side(st[NC, xc + 1, rows, :], st[NC + 1, xc + 1, rows, :], trans[0]),
            side(
                st[NC, xc, down_rows, :],
                st[NC + 1, xc, down_rows, :],
                trans[1],
            ),
            side(
                st[NC, xc, up_rows, :],
                st[NC + 1, xc, up_rows, :],
                trans[1],
            ),
            side(
                pltpu.roll(p, 1, 1),
                pltpu.roll(k, 1, 1),
                jnp.where(lane_id > 0, trans[2], 0.0),
            ),
            side(
                pltpu.roll(p, LANES - 1, 1),
                pltpu.roll(k, LANES - 1, 1),
                jnp.where(lane_id < LANES - 1, trans[2], 0.0),
            ),
        ]
        diag = pore_v[x]
        for out, _in in faces:
            diag = diag + out
        coming = [f[1] for f in faces]
        for i in range(NC):
            c = st[i, xc, rows, :]
            r = c * diag - old_v[i, x]
            r = r + coming[0] * st[i, xc - 1, rows, :]
            r = r + coming[1] * st[i, xc + 1, rows, :]
            r = r + coming[2] * st[i, xc, down_rows, :]
            r = r + coming[3] * st[i, xc, up_rows, :]
            r = r + coming[4] * pltpu.roll(c, 1, 1)
            r = r + coming[5] * pltpu.roll(c, LANES - 1, 1)
            resid_ref[i, x] = r
        return 0

    lax.fori_loop(0, CX, flux, 0)

    def post_line(k, _):
        first = jnp.maximum(s + 1, k * LINE)
        pl.semaphore_wait(ready.at[k], (k + 1) * LINE - first)
        lax.fori_loop(first, (k + 1) * LINE, post, 0)
        return 0

    lax.fori_loop((s + 1) // LINE, n_sub // LINE, post_line, 0)
    for there, copy in zip(sends, halo_copies):
        pl.when(there)(copy.wait_send)
    mail.wait_send()

    mail.wait_recv()
    table = mail_in[...].reshape(n_sub, LANES)
    p_seg = pick_rows(table, seg_hot_3, slot_hot > 0.5, 2)
    push = strength * (p_cell - p_seg)
    push_up, push_down = jnp.maximum(push, 0.0), jnp.minimum(push, 0.0)
    spread = jnp.concatenate([lane_hot * push_up, lane_hot * push_down], axis=0)
    dense = None
    for part in pieces_of(spread, 2):
        found = mm_nt(row_hot_b, part)
        dense = found if dense is None else dense + found
    wp_v[...] = dense[:, :LANES].reshape(CX, CY, LANES)
    wn_v[...] = dense[:, LANES:].reshape(CX, CY, LANES)

    mine = jnp.sum(table, axis=0, keepdims=True)
    row_v[...] = jnp.broadcast_to(mine, tile)
    rate = row_v[:, 32:64] - (cpp - 1.0) * row_v[:, 0:32]
    running = mm_full(rate, before_hot)
    well = base - friction[0] * running * jnp.abs(running)
    well_ref[...] = well[0:1]

    def perforated(x, _):
        wp, gain = wp_v[x], mob_v[x] * wn_v[x]
        for i in range(NC):
            v = inj_t[i]
            inj = jnp.concatenate([v, v], axis=0)
            resid_ref[i, x] = resid_ref[i, x] + (st[i, x + 1, rows, :] * wp + gain * inj)
        return 0

    lax.fori_loop(0, CX, perforated, 0)


def put(resid, lnphi, well, resid_out, lnphi_out, well_out, sem):
    pairs = ((resid, resid_out), (lnphi, lnphi_out), (well, well_out))
    copies = [pltpu.make_async_copy(a, b, sem.at[i]) for i, (a, b) in enumerate(pairs)]
    for copy in copies:
        copy.start()
    for copy in copies:
        copy.wait()


def per_device(n_grp, n_sub, *args):
    (
        amounts,
        pressure,
        heat,
        flag,
        perm,
        pore,
        former,
        trans,
        visc,
        crit,
        attract,
        covol,
        kappa,
        kij,
        recipe,
        locale,
        member,
        piece,
        strength,
        place,
        order,
        seg_pressure,
        exit_pressure,
        friction,
    ) = args
    field = (CX, CY, LANES)
    every = (NC, CX, CY, LANES)
    hbm = pl.BlockSpec(memory_space=pltpu.HBM)
    smem = pl.BlockSpec(memory_space=pltpu.SMEM)
    vmem = pl.BlockSpec(memory_space=pltpu.VMEM)
    mail = pltpu.VMEM((n_sub, 1, LANES), F32)
    one = pltpu.VMEM((8, LANES), F32)
    table = pltpu.VMEM((NC, 8, LANES), F32)
    edge = pltpu.VMEM((NC + 2, CX, LANES), F32)
    scratch = [
        pltpu.VMEM(every, F32),
        pltpu.VMEM(field, F32),
        pltpu.VMEM(field, jnp.int32),
        pltpu.VMEM(field, F32),
        pltpu.VMEM(every, F32),
        pltpu.VMEM((NC + 2, CX + 2, CY + 16, LANES), F32),
        pltpu.VMEM(every, F32),
        pltpu.VMEM(every, F32),
        *[pltpu.VMEM(field, F32) for _ in range(13)],
        table,
        table,
        table,
        table,
        one,
        mail,
        mail,
        edge,
        edge,
        edge,
        edge,
        pltpu.SemaphoreType.DMA((8,)),
        pltpu.SemaphoreType.DMA,
        pltpu.SemaphoreType.DMA,
        pltpu.SemaphoreType.REGULAR((n_sub // LINE,)),
        pltpu.SemaphoreType.DMA((4,)),
        pltpu.SemaphoreType.DMA((4,)),
        pltpu.SemaphoreType.DMA((SMALL,)),
    ]
    small = (
        trans,
        visc,
        crit,
        attract,
        covol,
        kappa,
        kij,
        recipe,
        locale.reshape(2, LANES),
        member.reshape(2, LANES),
        piece.reshape(2, LANES),
        strength.reshape(2, LANES),
        place,
        order,
        seg_pressure,
    )
    spaces = [pltpu.SMEM] * SCALARS + [pltpu.VMEM] * (SMALL - SCALARS)
    held = [space(v.shape, v.dtype) for space, v in zip(spaces, small)]
    outs = (
        jax.ShapeDtypeStruct(every, F32),
        jax.ShapeDtypeStruct(every, BF16),
        jax.ShapeDtypeStruct((1, 32), F32),
    )
    found = pl.pallas_call(
        functools.partial(body, n_grp, n_sub),
        out_shape=outs,
        in_specs=[hbm] * (7 + SMALL) + [smem] * 2,
        out_specs=(vmem, vmem, vmem),
        scratch_shapes=held + scratch,
        compiler_params=pltpu.CompilerParams(
            collective_id=0, has_side_effects=True, vmem_limit_bytes=40 * 1024 * 1024
        ),
        name="newton_residual",
    )(
        *[
            pltpu.with_memory_space_constraint(v, pltpu.HBM)
            for v in (amounts, pressure, heat, flag, perm, pore, former, *small)
        ],
        exit_pressure,
        friction,
    )
    return pl.pallas_call(
        put,
        out_shape=outs,
        in_specs=[vmem] * 3,
        out_specs=(hbm,) * 3,
        scratch_shapes=[pltpu.SemaphoreType.DMA((3,))],
        compiler_params=pltpu.CompilerParams(vmem_limit_bytes=4 * 1024 * 1024),
        name="put_outputs",
    )(*found)


def solution(mesh):
    areal = P("grp", "sub", None)
    every = P(None, "grp", "sub", None)
    both = P(("grp", "sub"))
    rows = P(("grp", "sub"), None)
    in_specs = (
        every,
        areal,
        areal,
        areal,
        areal,
        areal,
        every,
        *[P()] * 8,
        both,
        rows,
        both,
        both,
        P("grp", None),
        rows,
        rows,
        both,
        both,
    )
    return jax.shard_map(
        functools.partial(per_device, mesh.shape["grp"], mesh.shape["sub"]),
        mesh=mesh,
        in_specs=in_specs,
        out_specs=(every, every, rows),
        check_vma=False,
    )
```

```python
import functools
import math

import jax
import jax.numpy as jnp
from jax import lax
from jax.experimental import pallas as pl
from jax.experimental.pallas import tpu as pltpu
from jax.sharding import PartitionSpec as P

NEWT = 8
ROOT_TWO = math.sqrt(2.0)
MESH = pl.DeviceIdType.MESH
NC = 16
CX = 8
CY = 16
LANES = 128
LINE = 8
SMALL = 15
SCALARS = 8
F32 = jnp.float32
BF16 = jnp.bfloat16
HIGHEST = lax.Precision.HIGHEST


def iota(shape, axis):
    return lax.broadcasted_iota(jnp.int32, shape, axis)


def hot(index_row, rows):
    mask = iota((rows, index_row.shape[1]), 0) == index_row
    return jnp.where(mask, 1.0, 0.0).astype(F32)


def pieces_of(x, count):
    out = []
    for _ in range(count):
        top = x.astype(BF16)
        out.append(top)
        x = x - top.astype(F32)
    return out


def mm(a, b):
    return lax.dot_general(a, b, (((1,), (0,)), ((), ())), preferred_element_type=F32)


def mm_nt(a, b):
    return lax.dot_general(a, b, (((1,), (1,)), ((), ())), preferred_element_type=F32)


def mm_full(a, b):
    return lax.dot_general(
        a, b, (((1,), (0,)), ((), ())), precision=HIGHEST, preferred_element_type=F32
    )


def mm_full_nt(a, b):
    return lax.dot_general(
        a, b, (((1,), (1,)), ((), ())), precision=HIGHEST, preferred_element_type=F32
    )


def pick_rows(field, lane_hot, row_mask, count):
    parts = pieces_of(field, count)
    found = mm(jnp.concatenate(parts, axis=0), lane_hot)
    rows = field.shape[0]
    total = found[:rows]
    for i in range(1, count):
        total = total + found[i * rows : (i + 1) * rows]
    return jnp.sum(jnp.where(row_mask, total, 0.0), axis=0, keepdims=True)


def body(
    n_grp,
    n_sub,
    n_hbm,
    p_hbm,
    t_hbm,
    flag_hbm,
    k_hbm,
    pore_hbm,
    old_hbm,
    *refs,
):
    small_hbm, refs = refs[:SMALL], refs[SMALL:]
    exit_p, friction, *refs = refs
    resid_ref, lnphi_ref, well_ref, st, wp_v, gin_v, inj_t = refs[:7]
    small_refs, refs = refs[7 : 7 + SMALL], refs[7 + SMALL :]
    (
        trans,
        visc,
        crit,
        attract,
        covol,
        kappa,
        kij,
        recipe,
        loc_ref,
        mem_ref,
        seg_ref,
        wi_ref,
        gmp_ref,
        order_ref,
        cpp_ref,
    ) = small_refs
    (
        n_v,
        t_v,
        flag_v,
        pore_v,
        old_v,
        up_v,
        w_v,
        mob_v,
        e1_v,
        e2_v,
        e3_v,
        root_v,
        inv_v,
        pt_v,
        gain_v,
        a_v,
        b_v,
        z_v,
        c0_t,
        c1_t,
        cb_t,
        row_v,
        mail_out,
        mail_in,
        ys_lo,
        ys_hi,
        yr_lo,
        yr_hi,
        in_sem,
        mail_send,
        mail_recv,
        ready,
        halo_send,
        halo_recv,
        small_sem,
    ) = refs
    g = lax.axis_index("grp")
    s = lax.axis_index("sub")
    g_up, g_down = {"grp": (g + 1) % n_grp}, {"grp": (g + n_grp - 1) % n_grp}
    s_up, s_down = {"sub": (s + 1) % n_sub}, {"sub": (s + n_sub - 1) % n_sub}
    line = s // LINE
    has_g_up, has_g_down = g < n_grp - 1, g > 0
    has_s_up, has_s_down = s < n_sub - 1, s > 0

    inner = pl.ds(1, CX)
    rows = pl.ds(8, CY)
    half = CX // 2
    loads = [
        pltpu.make_async_copy(t_hbm, t_v, in_sem.at[0]),
        pltpu.make_async_copy(p_hbm, st.at[NC, inner, rows], in_sem.at[1]),
        pltpu.make_async_copy(n_hbm.at[:, pl.ds(0, half)], n_v.at[:, pl.ds(0, half)], in_sem.at[2]),
        pltpu.make_async_copy(
            n_hbm.at[:, pl.ds(half, half)], n_v.at[:, pl.ds(half, half)], in_sem.at[3]
        ),
        pltpu.make_async_copy(flag_hbm, flag_v, in_sem.at[4]),
        pltpu.make_async_copy(k_hbm, st.at[NC + 1, inner, rows], in_sem.at[5]),
        pltpu.make_async_copy(pore_hbm, pore_v, in_sem.at[6]),
        pltpu.make_async_copy(old_hbm, old_v, in_sem.at[7]),
    ]
    small_loads = [
        pltpu.make_async_copy(src, dst, small_sem.at[i])
        for i, (src, dst) in enumerate(zip(small_hbm, small_refs))
    ]
    for load in small_loads + loads[:4]:
        load.start()

    barrier = pltpu.get_barrier_semaphore()

    def greet(there, peer):
        @pl.when(there)
        def _():
            pl.semaphore_signal(barrier, inc=1, device_id=peer, device_id_type=MESH)

    def greet_higher(j, _):
        pl.semaphore_signal(barrier, inc=1, device_id={"sub": j}, device_id_type=MESH)
        return 0

    greet(has_g_up, g_up)
    greet(has_g_down, g_down)
    greet(has_s_down, s_down)
    lax.fori_loop(s + 1, n_sub, greet_higher, 0)
    expected = (
        s
        + has_s_up.astype(jnp.int32)
        + has_g_up.astype(jnp.int32)
        + has_g_down.astype(jnp.int32)
    )
    for load in loads[4:]:
        load.start()

    for load in small_loads:
        load.wait()

    tile = (8, LANES)
    for i in range(NC):
        amount = jnp.sqrt(jnp.full(tile, attract[i], F32))
        slope = jnp.full(tile, kappa[i], F32)
        c0_t[i] = amount * (1.0 + slope)
        c1_t[i] = amount * slope / jnp.sqrt(jnp.full(tile, crit[i], F32))
        cb_t[i] = jnp.full(tile, covol[i], F32)

    row_v[...] = jnp.zeros(tile, F32)
    row_v[0:1, 64:96] = cpp_ref[...] - 1.0
    own_row = row_v[0:1, :]

    loc = [loc_ref[h : h + 1, :] for h in range(2)]
    row_of = jnp.concatenate([v // LANES for v in loc], axis=1)
    lane_of = jnp.concatenate([v % LANES for v in loc], axis=1)
    member = jnp.concatenate([mem_ref[h : h + 1, :] for h in range(2)], axis=1)
    segment = jnp.concatenate([seg_ref[h : h + 1, :] for h in range(2)], axis=1)
    strength = jnp.concatenate([wi_ref[h : h + 1, :] for h in range(2)], axis=1)
    wells = n_sub
    place = jnp.where(iota((wells, wells), 0) == gmp_ref[...], 1.0, 0.0).astype(BF16)
    slot_hot = mm(place, hot(member, wells).astype(BF16))
    lane_hot = hot(lane_of, LANES)
    lane_hot_b = lane_hot.astype(BF16)
    row_mask = iota((LANES, 2 * LANES), 0) == row_of
    row_hot_b = jnp.where(row_mask, 1.0, 0.0).astype(BF16)
    seg_hot = hot(segment, LANES).astype(BF16)
    seg_hot_2 = hot(segment + 32, LANES).astype(BF16)
    seg_hot_3 = hot(segment + 64, LANES).astype(BF16)

    def wide(table, i):
        v = table[i]
        return jnp.broadcast_to(jnp.concatenate([v, v], axis=0)[None], (half, CY, LANES))

    loads[0].wait()
    loads[1].wait()

    def phase(b, _):
        xs = pl.ds(b * half, half)
        xp = pl.ds(b * half + 1, half)
        pltpu.make_async_copy(n_hbm.at[:, xs], n_v.at[:, xs], in_sem.at[2 + b]).wait()
        t = t_v[xs]
        root_t = jnp.sqrt(t)
        root_v[xs] = root_t
        whole = jnp.zeros_like(t)
        bsum = jnp.zeros_like(t)
        for i in range(NC):
            n = n_v[i, xs]
            w_v[i, xs] = n * jnp.abs(wide(c0_t, i) - wide(c1_t, i) * root_t)
            whole = whole + n
            bsum = bsum + wide(cb_t, i) * n
        last = w_v[NC - 1, xs]
        asum = last * last
        for i in range(NC - 1):
            m = None
            for j in range(i + 1, NC):
                term = w_v[j, xs] * (1.0 - kij[i, j])
                m = term if m is None else m + term
            up_v[i, xs] = m
            w = w_v[i, xs]
            asum = asum + w * (w + 2.0 * m)
        inv = 1.0 / whole
        inv_t = 1.0 / t
        pt = st[NC, xp, rows, :] * inv_t
        gain = pt * inv_t * inv
        inv_v[xs] = inv
        pt_v[xs] = pt
        gain_v[xs] = gain
        a_v[xs] = gain * inv * asum
        b_v[xs] = pt * inv * bsum
        return 0

    lax.fori_loop(0, 2, phase, 0)

    loads[4].wait()
    big_a, big_b = a_v[...], b_v[...]
    liquid = flag_v[...] == 1
    zed = jnp.where(liquid, big_b + 0.01, 1.0 + big_b)
    c1 = big_a - 3.0 * big_b * big_b - 2.0 * big_b
    c0 = big_b * big_b + big_b * big_b * big_b - big_a * big_b
    for _step in range(NEWT):
        c2 = big_b - 1.0
        value = ((zed + c2) * zed + c1) * zed + c0
        slope = (3.0 * zed + 2.0 * c2) * zed + c1
        zed = jnp.maximum(zed - value / jnp.maximum(slope, 0.1), big_b + 0.01)
    z_v[...] = zed
    mob_v[...] = pt_v[...] / (zed * jnp.where(liquid, visc[1], visc[0]))

    p_cell = pick_rows(
        st[NC, inner, rows, :].reshape(LANES, LANES) - 1.0, lane_hot_b, row_mask, 2
    )
    mob_cell = pick_rows(mob_v[...].reshape(LANES, LANES), lane_hot_b, row_mask, 2)
    v0 = strength * mob_cell
    v1 = v0 * p_cell
    left = jnp.concatenate([slot_hot * v0, slot_hot * v1], axis=1)
    right = jnp.concatenate([seg_hot, seg_hot_2], axis=1)
    sums = None
    for part in pieces_of(left, 2):
        found = mm_nt(part, right)
        sums = found if sums is None else sums + found
    mail_out[...] = (sums + own_row).reshape(n_sub, 1, LANES)
    mail_in[s] = mail_out[s]

    def post(j, _):
        pltpu.make_async_remote_copy(
            src_ref=mail_out.at[j],
            dst_ref=mail_in.at[s],
            send_sem=mail_send,
            recv_sem=mail_recv,
            device_id={"sub": j},
            device_id_type=MESH,
        ).start()
        return 0

    def post_lower(j, _):
        post(j, 0)
        pl.semaphore_signal(
            ready.at[line], inc=1, device_id={"sub": j}, device_id_type=MESH
        )
        return 0

    pl.semaphore_wait(barrier, expected)
    lax.fori_loop(0, s, post_lower, 0)
    mail = pltpu.make_async_remote_copy(
        src_ref=mail_out.at[pl.ds(0, n_sub - 1)],
        dst_ref=mail_in.at[pl.ds(0, n_sub - 1)],
        send_sem=mail_send,
        recv_sem=mail_recv,
        device_id=g_up,
        device_id_type=MESH,
    )

    def carry(x, _):
        share = mob_v[x] * inv_v[x]
        for i in range(NC):
            st[i, x + 1, rows, :] = n_v[i, x] * share
        return 0

    lax.fori_loop(0, CX, carry, 0)
    loads[5].wait()

    def gather_rows(c, _):
        ys_lo[c] = st[c, inner, 8, :]
        ys_hi[c] = st[c, inner, 8 + CY - 1, :]
        return 0

    lax.fori_loop(0, NC + 2, gather_rows, 0)

    def halo_copy(src, dst, slot, peer):
        return pltpu.make_async_remote_copy(
            src_ref=src,
            dst_ref=dst,
            send_sem=halo_send.at[slot],
            recv_sem=halo_recv.at[slot],
            device_id=peer,
            device_id_type=MESH,
        )

    halo_copies = [
        halo_copy(st.at[:, CX, rows], st.at[:, 0, rows], 0, g_up),
        halo_copy(st.at[:, 1, rows], st.at[:, CX + 1, rows], 1, g_down),
        halo_copy(ys_hi, yr_lo, 2, s_up),
        halo_copy(ys_lo, yr_hi, 3, s_down),
    ]
    sends = (has_g_up, has_g_down, has_s_up, has_s_down)
    receives = (has_g_down, has_g_up, has_s_down, has_s_up)

    for there, copy in zip(sends, halo_copies):
        pl.when(there)(copy.start)

    @pl.when(jnp.logical_not(has_g_down))
    def _():
        st[:, 0, rows, :] = jnp.zeros((NC + 2, CY, LANES), F32)

    @pl.when(jnp.logical_not(has_g_up))
    def _():
        st[:, CX + 1, rows, :] = jnp.zeros((NC + 2, CY, LANES), F32)

    @pl.when(jnp.logical_not(has_s_down))
    def _():
        yr_lo[...] = jnp.zeros((NC + 2, CX, LANES), F32)

    @pl.when(jnp.logical_not(has_s_up))
    def _():
        yr_hi[...] = jnp.zeros((NC + 2, CX, LANES), F32)

    total = jnp.zeros(tile, F32)
    for i in range(NC):
        total = total + recipe[i]
    for i in range(NC):
        inj_t[i] = jnp.full(tile, recipe[i], F32) / total

    order = jnp.where(iota((32, 32), 0) == order_ref[...], 1.0, 0.0).astype(F32)
    sub32, lane32 = iota((32, 32), 0), iota((32, 32), 1)
    upper = jnp.where(sub32 <= lane32, 1.0, 0.0).astype(F32)
    after = jnp.where(sub32 == lane32 + 1, 1.0, 0.0).astype(F32)
    before_hot = mm_full_nt(mm_full(order, upper), order)
    next_hot = mm_full_nt(mm_full(order, after), order)
    last_row = jnp.where(iota((8, 32), 1) == 31, 1.0, 0.0).astype(F32)
    last_hot = mm_full_nt(last_row, order)
    cpp = jnp.broadcast_to(cpp_ref[...], (8, 32))
    base = cpp - (mm_full(cpp, next_hot) + exit_p[0] * last_hot)


    loads[6].wait()

    def fugacity(b, _):
        xs = pl.ds(b * half, half)
        zed, big_b, pt = z_v[xs], b_v[xs], pt_v[xs]
        ratio = jnp.log((zed + (1.0 + ROOT_TWO) * big_b) / (zed + (1.0 - ROOT_TWO) * big_b))
        inv_b = 1.0 / big_b
        e3 = ratio * inv_b * (1.0 / ROOT_TWO)
        e1_v[xs] = pt * inv_b * ((zed - 1.0) + 0.5 * a_v[xs] * e3)
        e2_v[xs] = jnp.log(zed - big_b)
        e3_v[xs] = e3 * gain_v[xs]
        pore_v[xs] = pore_v[xs] * jnp.where(flag_v[xs] == 1, visc[1], visc[0])
        for i in range(NC):
            m = w_v[i, xs]
            if i < NC - 1:
                m = m + up_v[i, xs]
            for j in range(i):
                m = m + w_v[j, xs] * (1.0 - kij[i, j])
            u = jnp.abs(wide(c0_t, i) - wide(c1_t, i) * root_v[xs])
            part = wide(cb_t, i) * e1_v[xs] - e2_v[xs]
            lnphi_ref[i, xs] = (part - u * m * e3_v[xs]).astype(BF16)
        return 0

    lax.fori_loop(0, 2, fugacity, 0)

    for there, copy in zip(receives, halo_copies):
        pl.when(there)(copy.wait_recv)

    def put_rows(c, _):
        st[c, inner, 7, :] = yr_lo[c]
        st[c, inner, 8 + CY, :] = yr_hi[c]
        return 0

    lax.fori_loop(0, NC + 2, put_rows, 0)
    loads[7].wait()

    plane = (CY, LANES)
    lane_id = iota(plane, 1)

    def flux(x, _):
        xc = x + 1
        p, k = st[NC, xc, rows, :], st[NC + 1, xc, rows, :]

        def side(p_b, k_b, factor):
            trans_ab = factor * 2.0 * k * k_b / (k + k_b)
            flow = trans_ab * (p - p_b)
            return jnp.maximum(flow, 0.0), jnp.minimum(flow, 0.0)

        up_rows, down_rows = pl.ds(9, CY), pl.ds(7, CY)
        faces = [
            side(st[NC, xc - 1, rows, :], st[NC + 1, xc - 1, rows, :], trans[0]),
            side(st[NC, xc + 1, rows, :], st[NC + 1, xc + 1, rows, :], trans[0]),
            side(
                st[NC, xc, down_rows, :],
                st[NC + 1, xc, down_rows, :],
                trans[1],
            ),
            side(
                st[NC, xc, up_rows, :],
                st[NC + 1, xc, up_rows, :],
                trans[1],
            ),
            side(
                pltpu.roll(p, 1, 1),
                pltpu.roll(k, 1, 1),
                jnp.where(lane_id > 0, trans[2], 0.0),
            ),
            side(
                pltpu.roll(p, LANES - 1, 1),
                pltpu.roll(k, LANES - 1, 1),
                jnp.where(lane_id < LANES - 1, trans[2], 0.0),
            ),
        ]
        diag = pore_v[x]
        for out, _in in faces:
            diag = diag + out
        coming = [f[1] for f in faces]
        for i in range(NC):
            c = st[i, xc, rows, :]
            r = c * diag - old_v[i, x]
            r = r + coming[0] * st[i, xc - 1, rows, :]
            r = r + coming[1] * st[i, xc + 1, rows, :]
            r = r + coming[2] * st[i, xc, down_rows, :]
            r = r + coming[3] * st[i, xc, up_rows, :]
            r = r + coming[4] * pltpu.roll(c, 1, 1)
            r = r + coming[5] * pltpu.roll(c, LANES - 1, 1)
            resid_ref[i, x] = r
        return 0

    lax.fori_loop(0, CX, flux, 0)

    def post_line(k, _):
        first = jnp.maximum(s + 1, k * LINE)
        pl.semaphore_wait(ready.at[k], (k + 1) * LINE - first)
        lax.fori_loop(first, (k + 1) * LINE, post, 0)
        return 0

    lax.fori_loop((s + 1) // LINE, n_sub // LINE, post_line, 0)
    for there, copy in zip(sends, halo_copies):
        pl.when(there)(copy.wait_send)
    mail.wait_send()

    mail.wait_recv()
    table = mail_in[...].reshape(n_sub, LANES)
    p_seg = pick_rows(table, seg_hot_3, slot_hot > 0.5, 2)
    push = strength * (p_cell - p_seg)
    push_up, push_down = jnp.maximum(push, 0.0), jnp.minimum(push, 0.0)
    spread = jnp.concatenate([lane_hot * push_up, lane_hot * push_down], axis=0)
    dense = None
    for part in pieces_of(spread, 2):
        found = mm_nt(row_hot_b, part)
        dense = found if dense is None else dense + found
    wp_v[...] = dense[:, :LANES].reshape(CX, CY, LANES)
    gin_v[...] = mob_v[...] * dense[:, LANES:].reshape(CX, CY, LANES)

    inflow = jnp.sum(table, axis=0, keepdims=True)
    row_v[...] = jnp.broadcast_to(inflow, tile)
    rate = row_v[:, 32:64] - (cpp - 1.0) * row_v[:, 0:32]
    running = mm_full(rate, before_hot)
    well = base - friction[0] * running * jnp.abs(running)
    well_ref[...] = well[0:1]


def put(resid, lnphi, well, st, wp, gin, inj, resid_out, lnphi_out, well_out, done, sem):
    others = [
        pltpu.make_async_copy(lnphi, lnphi_out, sem.at[CX]),
        pltpu.make_async_copy(well, well_out, sem.at[CX + 1]),
    ]
    for copy in others:
        copy.start()
    planes = []
    for x in range(CX):
        for i in range(NC):
            v = inj[i]
            into = gin[x] * jnp.concatenate([v, v], axis=0)
            out = st[i, x + 1, pl.ds(8, CY), :] * wp[x]
            done[i, x] = resid[i, x] + (out + into)
        planes.append(pltpu.make_async_copy(done.at[:, x], resid_out.at[:, x], sem.at[x]))
        planes[-1].start()
    for copy in planes + others:
        copy.wait()


def per_device(n_grp, n_sub, *args):
    (
        amounts,
        pressure,
        heat,
        flag,
        perm,
        pore,
        former,
        trans,
        visc,
        crit,
        attract,
        covol,
        kappa,
        kij,
        recipe,
        locale,
        member,
        piece,
        strength,
        place,
        order,
        seg_pressure,
        exit_pressure,
        friction,
    ) = args
    field = (CX, CY, LANES)
    every = (NC, CX, CY, LANES)
    hbm = pl.BlockSpec(memory_space=pltpu.HBM)
    smem = pl.BlockSpec(memory_space=pltpu.SMEM)
    vmem = pl.BlockSpec(memory_space=pltpu.VMEM)
    mail = pltpu.VMEM((n_sub, 1, LANES), F32)
    one = pltpu.VMEM((8, LANES), F32)
    table = pltpu.VMEM((NC, 8, LANES), F32)
    edge = pltpu.VMEM((NC + 2, CX, LANES), F32)
    scratch = [
        pltpu.VMEM(every, F32),
        pltpu.VMEM(field, F32),
        pltpu.VMEM(field, jnp.int32),
        pltpu.VMEM(field, F32),
        pltpu.VMEM(every, F32),
        pltpu.VMEM(every, F32),
        pltpu.VMEM(every, F32),
        *[pltpu.VMEM(field, F32) for _ in range(11)],
        table,
        table,
        table,
        one,
        mail,
        mail,
        edge,
        edge,
        edge,
        edge,
        pltpu.SemaphoreType.DMA((8,)),
        pltpu.SemaphoreType.DMA,
        pltpu.SemaphoreType.DMA,
        pltpu.SemaphoreType.REGULAR((n_sub // LINE,)),
        pltpu.SemaphoreType.DMA((4,)),
        pltpu.SemaphoreType.DMA((4,)),
        pltpu.SemaphoreType.DMA((SMALL,)),
    ]
    small = (
        trans,
        visc,
        crit,
        attract,
        covol,
        kappa,
        kij,
        recipe,
        locale.reshape(2, LANES),
        member.reshape(2, LANES),
        piece.reshape(2, LANES),
        strength.reshape(2, LANES),
        place,
        order,
        seg_pressure,
    )
    spaces = [pltpu.SMEM] * SCALARS + [pltpu.VMEM] * (SMALL - SCALARS)
    held = [space(v.shape, v.dtype) for space, v in zip(spaces, small)]
    outs = (
        jax.ShapeDtypeStruct(every, F32),
        jax.ShapeDtypeStruct(every, BF16),
        jax.ShapeDtypeStruct((1, 32), F32),
    )
    found = pl.pallas_call(
        functools.partial(body, n_grp, n_sub),
        out_shape=(
            *outs,
            jax.ShapeDtypeStruct((NC + 2, CX + 2, CY + 16, LANES), F32),
            jax.ShapeDtypeStruct(field, F32),
            jax.ShapeDtypeStruct(field, F32),
            jax.ShapeDtypeStruct((NC, 8, LANES), F32),
        ),
        in_specs=[hbm] * (7 + SMALL) + [smem] * 2,
        out_specs=(vmem,) * 7,
        scratch_shapes=held + scratch,
        compiler_params=pltpu.CompilerParams(
            collective_id=0, has_side_effects=True, vmem_limit_bytes=40 * 1024 * 1024
        ),
        name="newton_residual",
    )(
        *[
            pltpu.with_memory_space_constraint(v, pltpu.HBM)
            for v in (amounts, pressure, heat, flag, perm, pore, former, *small)
        ],
        exit_pressure,
        friction,
    )
    return pl.pallas_call(
        put,
        out_shape=outs,
        in_specs=[vmem] * 7,
        out_specs=(hbm,) * 3,
        scratch_shapes=[pltpu.VMEM(every, F32), pltpu.SemaphoreType.DMA((CX + 2,))],
        compiler_params=pltpu.CompilerParams(vmem_limit_bytes=8 * 1024 * 1024),
        name="put_outputs",
    )(*found)


def solution(mesh):
    areal = P("grp", "sub", None)
    every = P(None, "grp", "sub", None)
    both = P(("grp", "sub"))
    rows = P(("grp", "sub"), None)
    in_specs = (
        every,
        areal,
        areal,
        areal,
        areal,
        areal,
        every,
        *[P()] * 8,
        both,
        rows,
        both,
        both,
        P("grp", None),
        rows,
        rows,
        both,
        both,
    )
    return jax.shard_map(
        functools.partial(per_device, mesh.shape["grp"], mesh.shape["sub"]),
        mesh=mesh,
        in_specs=in_specs,
        out_specs=(every, every, rows),
        check_vma=False,
    )
```

```python
import functools
import math

import jax
import jax.numpy as jnp
from jax import lax
from jax.experimental import pallas as pl
from jax.experimental.pallas import tpu as pltpu
from jax.sharding import PartitionSpec as P

NEWT = 8
ROOT_TWO = math.sqrt(2.0)
MESH = pl.DeviceIdType.MESH
NC = 16
CX = 8
CY = 16
LANES = 128
LINE = 8
SMALL = 15
SCALARS = 8
F32 = jnp.float32
BF16 = jnp.bfloat16
HIGHEST = lax.Precision.HIGHEST


def iota(shape, axis):
    return lax.broadcasted_iota(jnp.int32, shape, axis)


def hot(index_row, rows):
    mask = iota((rows, index_row.shape[1]), 0) == index_row
    return jnp.where(mask, 1.0, 0.0).astype(F32)


def pieces_of(x, count):
    out = []
    for _ in range(count):
        top = x.astype(BF16)
        out.append(top)
        x = x - top.astype(F32)
    return out


def mm(a, b):
    return lax.dot_general(a, b, (((1,), (0,)), ((), ())), preferred_element_type=F32)


def mm_nt(a, b):
    return lax.dot_general(a, b, (((1,), (1,)), ((), ())), preferred_element_type=F32)


def mm_full(a, b):
    return lax.dot_general(
        a, b, (((1,), (0,)), ((), ())), precision=HIGHEST, preferred_element_type=F32
    )


def mm_full_nt(a, b):
    return lax.dot_general(
        a, b, (((1,), (1,)), ((), ())), precision=HIGHEST, preferred_element_type=F32
    )


def pick_rows(field, lane_hot, row_mask, count):
    parts = pieces_of(field, count)
    found = mm(jnp.concatenate(parts, axis=0), lane_hot)
    rows = field.shape[0]
    total = found[:rows]
    for i in range(1, count):
        total = total + found[i * rows : (i + 1) * rows]
    return jnp.sum(jnp.where(row_mask, total, 0.0), axis=0, keepdims=True)


def body(
    n_grp,
    n_sub,
    n_hbm,
    p_hbm,
    t_hbm,
    flag_hbm,
    k_hbm,
    pore_hbm,
    old_hbm,
    *refs,
):
    small_hbm, refs = refs[:SMALL], refs[SMALL:]
    exit_p, friction, *refs = refs
    resid_ref, lnphi_ref, well_ref, st, wp_v, gin_v, inj_t = refs[:7]
    small_refs, refs = refs[7 : 7 + SMALL], refs[7 + SMALL :]
    (
        trans,
        visc,
        crit,
        attract,
        covol,
        kappa,
        kij,
        recipe,
        loc_ref,
        mem_ref,
        seg_ref,
        wi_ref,
        gmp_ref,
        order_ref,
        cpp_ref,
    ) = small_refs
    (
        n_v,
        t_v,
        flag_v,
        pore_v,
        old_v,
        up_v,
        w_v,
        mob_v,
        e1_v,
        e2_v,
        e3_v,
        root_v,
        inv_v,
        pt_v,
        gain_v,
        a_v,
        b_v,
        z_v,
        c0_t,
        c1_t,
        cb_t,
        row_v,
        mail_out,
        mail_in,
        ys_lo,
        ys_hi,
        yr_lo,
        yr_hi,
        in_sem,
        mail_send,
        mail_recv,
        ready,
        halo_send,
        halo_recv,
        small_sem,
    ) = refs
    g = lax.axis_index("grp")
    s = lax.axis_index("sub")
    g_up, g_down = {"grp": (g + 1) % n_grp}, {"grp": (g + n_grp - 1) % n_grp}
    s_up, s_down = {"sub": (s + 1) % n_sub}, {"sub": (s + n_sub - 1) % n_sub}
    line = s // LINE
    has_g_up, has_g_down = g < n_grp - 1, g > 0
    has_s_up, has_s_down = s < n_sub - 1, s > 0

    inner = pl.ds(1, CX)
    rows = pl.ds(8, CY)
    half = CX // 2
    loads = [
        pltpu.make_async_copy(t_hbm, t_v, in_sem.at[0]),
        pltpu.make_async_copy(p_hbm, st.at[NC, inner, rows], in_sem.at[1]),
        pltpu.make_async_copy(n_hbm.at[:, pl.ds(0, half)], n_v.at[:, pl.ds(0, half)], in_sem.at[2]),
        pltpu.make_async_copy(
            n_hbm.at[:, pl.ds(half, half)], n_v.at[:, pl.ds(half, half)], in_sem.at[3]
        ),
        pltpu.make_async_copy(flag_hbm, flag_v, in_sem.at[4]),
        pltpu.make_async_copy(k_hbm, st.at[NC + 1, inner, rows], in_sem.at[5]),
        pltpu.make_async_copy(pore_hbm, pore_v, in_sem.at[6]),
        pltpu.make_async_copy(old_hbm, old_v, in_sem.at[7]),
    ]
    small_loads = [
        pltpu.make_async_copy(src, dst, small_sem.at[i])
        for i, (src, dst) in enumerate(zip(small_hbm, small_refs))
    ]
    for load in small_loads[:SCALARS] + loads[:4]:
        load.start()

    barrier = pltpu.get_barrier_semaphore()

    def greet(there, peer):
        @pl.when(there)
        def _():
            pl.semaphore_signal(barrier, inc=1, device_id=peer, device_id_type=MESH)

    def greet_higher(j, _):
        pl.semaphore_signal(barrier, inc=1, device_id={"sub": j}, device_id_type=MESH)
        return 0

    greet(has_g_up, g_up)
    greet(has_g_down, g_down)
    greet(has_s_down, s_down)
    lax.fori_loop(s + 1, n_sub, greet_higher, 0)
    expected = (
        s
        + has_s_up.astype(jnp.int32)
        + has_g_up.astype(jnp.int32)
        + has_g_down.astype(jnp.int32)
    )
    for load in small_loads[SCALARS:] + loads[4:]:
        load.start()

    for load in small_loads[:SCALARS]:
        load.wait()

    tile = (8, LANES)
    for i in range(NC):
        amount = jnp.sqrt(jnp.full(tile, attract[i], F32))
        slope = jnp.full(tile, kappa[i], F32)
        c0_t[i] = amount * (1.0 + slope)
        c1_t[i] = amount * slope / jnp.sqrt(jnp.full(tile, crit[i], F32))
        cb_t[i] = jnp.full(tile, covol[i], F32)

    def wide(table, i):
        v = table[i]
        return jnp.broadcast_to(jnp.concatenate([v, v], axis=0)[None], (half, CY, LANES))

    loads[0].wait()
    loads[1].wait()

    def phase(b, _):
        xs = pl.ds(b * half, half)
        xp = pl.ds(b * half + 1, half)
        pltpu.make_async_copy(n_hbm.at[:, xs], n_v.at[:, xs], in_sem.at[2 + b]).wait()
        t = t_v[xs]
        root_t = jnp.sqrt(t)
        root_v[xs] = root_t
        whole = jnp.zeros_like(t)
        bsum = jnp.zeros_like(t)
        for i in range(NC):
            n = n_v[i, xs]
            w_v[i, xs] = n * jnp.abs(wide(c0_t, i) - wide(c1_t, i) * root_t)
            whole = whole + n
            bsum = bsum + wide(cb_t, i) * n
        last = w_v[NC - 1, xs]
        asum = last * last
        for i in range(NC - 1):
            m = None
            for j in range(i + 1, NC):
                term = w_v[j, xs] * (1.0 - kij[i, j])
                m = term if m is None else m + term
            up_v[i, xs] = m
            w = w_v[i, xs]
            asum = asum + w * (w + 2.0 * m)
        inv = 1.0 / whole
        inv_t = 1.0 / t
        pt = st[NC, xp, rows, :] * inv_t
        gain = pt * inv_t * inv
        inv_v[xs] = inv
        pt_v[xs] = pt
        gain_v[xs] = gain
        a_v[xs] = gain * inv * asum
        b_v[xs] = pt * inv * bsum
        return 0

    lax.fori_loop(0, 2, phase, 0)

    for load in small_loads[SCALARS:]:
        load.wait()
    loads[4].wait()

    row_v[...] = jnp.zeros(tile, F32)
    row_v[0:1, 64:96] = cpp_ref[...] - 1.0
    own_row = row_v[0:1, :]

    loc = [loc_ref[h : h + 1, :] for h in range(2)]
    row_of = jnp.concatenate([v // LANES for v in loc], axis=1)
    lane_of = jnp.concatenate([v % LANES for v in loc], axis=1)
    member = jnp.concatenate([mem_ref[h : h + 1, :] for h in range(2)], axis=1)
    segment = jnp.concatenate([seg_ref[h : h + 1, :] for h in range(2)], axis=1)
    strength = jnp.concatenate([wi_ref[h : h + 1, :] for h in range(2)], axis=1)
    wells = n_sub
    place = jnp.where(iota((wells, wells), 0) == gmp_ref[...], 1.0, 0.0).astype(BF16)
    slot_hot = mm(place, hot(member, wells).astype(BF16))
    lane_hot = hot(lane_of, LANES)
    lane_hot_b = lane_hot.astype(BF16)
    row_mask = iota((LANES, 2 * LANES), 0) == row_of
    row_hot_b = jnp.where(row_mask, 1.0, 0.0).astype(BF16)
    seg_hot = hot(segment, LANES).astype(BF16)
    seg_hot_2 = hot(segment + 32, LANES).astype(BF16)
    seg_hot_3 = hot(segment + 64, LANES).astype(BF16)

    big_a, big_b = a_v[...], b_v[...]
    liquid = flag_v[...] == 1
    zed = jnp.where(liquid, big_b + 0.01, 1.0 + big_b)
    c1 = big_a - 3.0 * big_b * big_b - 2.0 * big_b
    c0 = big_b * big_b + big_b * big_b * big_b - big_a * big_b
    for _step in range(NEWT):
        c2 = big_b - 1.0
        value = ((zed + c2) * zed + c1) * zed + c0
        slope = (3.0 * zed + 2.0 * c2) * zed + c1
        zed = jnp.maximum(zed - value / jnp.maximum(slope, 0.1), big_b + 0.01)
    z_v[...] = zed
    mob_v[...] = pt_v[...] / (zed * jnp.where(liquid, visc[1], visc[0]))

    p_cell = pick_rows(
        st[NC, inner, rows, :].reshape(LANES, LANES) - 1.0, lane_hot_b, row_mask, 2
    )
    mob_cell = pick_rows(mob_v[...].reshape(LANES, LANES), lane_hot_b, row_mask, 2)
    v0 = strength * mob_cell
    v1 = v0 * p_cell
    left = jnp.concatenate([slot_hot * v0, slot_hot * v1], axis=1)
    right = jnp.concatenate([seg_hot, seg_hot_2], axis=1)
    sums = None
    for part in pieces_of(left, 2):
        found = mm_nt(part, right)
        sums = found if sums is None else sums + found
    mail_out[...] = (sums + own_row).reshape(n_sub, 1, LANES)
    mail_in[s] = mail_out[s]

    def post(j, _):
        pltpu.make_async_remote_copy(
            src_ref=mail_out.at[j],
            dst_ref=mail_in.at[s],
            send_sem=mail_send,
            recv_sem=mail_recv,
            device_id={"sub": j},
            device_id_type=MESH,
        ).start()
        return 0

    def post_lower(j, _):
        post(j, 0)
        pl.semaphore_signal(
            ready.at[line], inc=1, device_id={"sub": j}, device_id_type=MESH
        )
        return 0

    pl.semaphore_wait(barrier, expected)
    lax.fori_loop(0, s, post_lower, 0)
    mail = pltpu.make_async_remote_copy(
        src_ref=mail_out.at[pl.ds(0, n_sub - 1)],
        dst_ref=mail_in.at[pl.ds(0, n_sub - 1)],
        send_sem=mail_send,
        recv_sem=mail_recv,
        device_id=g_up,
        device_id_type=MESH,
    )

    loads[6].wait()

    def fugacity(b, _):
        xs = pl.ds(b * half, half)
        zed, big_b, pt = z_v[xs], b_v[xs], pt_v[xs]
        ratio = jnp.log((zed + (1.0 + ROOT_TWO) * big_b) / (zed + (1.0 - ROOT_TWO) * big_b))
        inv_b = 1.0 / big_b
        e3 = ratio * inv_b * (1.0 / ROOT_TWO)
        e1_v[xs] = pt * inv_b * ((zed - 1.0) + 0.5 * a_v[xs] * e3)
        e2_v[xs] = jnp.log(zed - big_b)
        e3_v[xs] = e3 * gain_v[xs]
        pore_v[xs] = pore_v[xs] * jnp.where(flag_v[xs] == 1, visc[1], visc[0])
        for i in range(NC):
            m = w_v[i, xs]
            if i < NC - 1:
                m = m + up_v[i, xs]
            for j in range(i):
                m = m + w_v[j, xs] * (1.0 - kij[i, j])
            u = jnp.abs(wide(c0_t, i) - wide(c1_t, i) * root_v[xs])
            part = wide(cb_t, i) * e1_v[xs] - e2_v[xs]
            lnphi_ref[i, xs] = (part - u * m * e3_v[xs]).astype(BF16)
        return 0

    lax.fori_loop(0, 2, fugacity, 0)

    def carry(x, _):
        share = mob_v[x] * inv_v[x]
        for i in range(NC):
            st[i, x + 1, rows, :] = n_v[i, x] * share
        return 0

    lax.fori_loop(0, CX, carry, 0)
    loads[5].wait()

    def gather_rows(c, _):
        ys_lo[c] = st[c, inner, 8, :]
        ys_hi[c] = st[c, inner, 8 + CY - 1, :]
        return 0

    lax.fori_loop(0, NC + 2, gather_rows, 0)

    def halo_copy(src, dst, slot, peer):
        return pltpu.make_async_remote_copy(
            src_ref=src,
            dst_ref=dst,
            send_sem=halo_send.at[slot],
            recv_sem=halo_recv.at[slot],
            device_id=peer,
            device_id_type=MESH,
        )

    halo_copies = [
        halo_copy(st.at[:, CX, rows], st.at[:, 0, rows], 0, g_up),
        halo_copy(st.at[:, 1, rows], st.at[:, CX + 1, rows], 1, g_down),
        halo_copy(ys_hi, yr_lo, 2, s_up),
        halo_copy(ys_lo, yr_hi, 3, s_down),
    ]
    sends = (has_g_up, has_g_down, has_s_up, has_s_down)
    receives = (has_g_down, has_g_up, has_s_down, has_s_up)

    for there, copy in zip(sends, halo_copies):
        pl.when(there)(copy.start)

    @pl.when(jnp.logical_not(has_g_down))
    def _():
        st[:, 0, rows, :] = jnp.zeros((NC + 2, CY, LANES), F32)

    @pl.when(jnp.logical_not(has_g_up))
    def _():
        st[:, CX + 1, rows, :] = jnp.zeros((NC + 2, CY, LANES), F32)

    @pl.when(jnp.logical_not(has_s_down))
    def _():
        yr_lo[...] = jnp.zeros((NC + 2, CX, LANES), F32)

    @pl.when(jnp.logical_not(has_s_up))
    def _():
        yr_hi[...] = jnp.zeros((NC + 2, CX, LANES), F32)

    total = jnp.zeros(tile, F32)
    for i in range(NC):
        total = total + recipe[i]
    for i in range(NC):
        inj_t[i] = jnp.full(tile, recipe[i], F32) / total

    order = jnp.where(iota((32, 32), 0) == order_ref[...], 1.0, 0.0).astype(F32)
    sub32, lane32 = iota((32, 32), 0), iota((32, 32), 1)
    upper = jnp.where(sub32 <= lane32, 1.0, 0.0).astype(F32)
    after = jnp.where(sub32 == lane32 + 1, 1.0, 0.0).astype(F32)
    before_hot = mm_full_nt(mm_full(order, upper), order)
    next_hot = mm_full_nt(mm_full(order, after), order)
    last_row = jnp.where(iota((8, 32), 1) == 31, 1.0, 0.0).astype(F32)
    last_hot = mm_full_nt(last_row, order)
    cpp = jnp.broadcast_to(cpp_ref[...], (8, 32))
    base = cpp - (mm_full(cpp, next_hot) + exit_p[0] * last_hot)


    for there, copy in zip(receives, halo_copies):
        pl.when(there)(copy.wait_recv)

    def put_rows(c, _):
        st[c, inner, 7, :] = yr_lo[c]
        st[c, inner, 8 + CY, :] = yr_hi[c]
        return 0

    lax.fori_loop(0, NC + 2, put_rows, 0)
    loads[7].wait()

    plane = (CY, LANES)
    lane_id = iota(plane, 1)

    def flux(x, _):
        xc = x + 1
        p, k = st[NC, xc, rows, :], st[NC + 1, xc, rows, :]

        def side(p_b, k_b, factor):
            trans_ab = factor * 2.0 * k * k_b / (k + k_b)
            flow = trans_ab * (p - p_b)
            return jnp.maximum(flow, 0.0), jnp.minimum(flow, 0.0)

        up_rows, down_rows = pl.ds(9, CY), pl.ds(7, CY)
        faces = [
            side(st[NC, xc - 1, rows, :], st[NC + 1, xc - 1, rows, :], trans[0]),
            side(st[NC, xc + 1, rows, :], st[NC + 1, xc + 1, rows, :], trans[0]),
            side(
                st[NC, xc, down_rows, :],
                st[NC + 1, xc, down_rows, :],
                trans[1],
            ),
            side(
                st[NC, xc, up_rows, :],
                st[NC + 1, xc, up_rows, :],
                trans[1],
            ),
            side(
                pltpu.roll(p, 1, 1),
                pltpu.roll(k, 1, 1),
                jnp.where(lane_id > 0, trans[2], 0.0),
            ),
            side(
                pltpu.roll(p, LANES - 1, 1),
                pltpu.roll(k, LANES - 1, 1),
                jnp.where(lane_id < LANES - 1, trans[2], 0.0),
            ),
        ]
        diag = pore_v[x]
        for out, _in in faces:
            diag = diag + out
        coming = [f[1] for f in faces]
        for i in range(NC):
            c = st[i, xc, rows, :]
            r = c * diag - old_v[i, x]
            r = r + coming[0] * st[i, xc - 1, rows, :]
            r = r + coming[1] * st[i, xc + 1, rows, :]
            r = r + coming[2] * st[i, xc, down_rows, :]
            r = r + coming[3] * st[i, xc, up_rows, :]
            r = r + coming[4] * pltpu.roll(c, 1, 1)
            r = r + coming[5] * pltpu.roll(c, LANES - 1, 1)
            resid_ref[i, x] = r
        return 0

    lax.fori_loop(0, CX, flux, 0)

    def post_line(k, _):
        first = jnp.maximum(s + 1, k * LINE)
        pl.semaphore_wait(ready.at[k], (k + 1) * LINE - first)
        lax.fori_loop(first, (k + 1) * LINE, post, 0)
        return 0

    lax.fori_loop((s + 1) // LINE, n_sub // LINE, post_line, 0)
    for there, copy in zip(sends, halo_copies):
        pl.when(there)(copy.wait_send)
    mail.wait_send()

    mail.wait_recv()
    table = mail_in[...].reshape(n_sub, LANES)
    p_seg = pick_rows(table, seg_hot_3, slot_hot > 0.5, 2)
    push = strength * (p_cell - p_seg)
    push_up, push_down = jnp.maximum(push, 0.0), jnp.minimum(push, 0.0)
    spread = jnp.concatenate([lane_hot * push_up, lane_hot * push_down], axis=0)
    dense = None
    for part in pieces_of(spread, 2):
        found = mm_nt(row_hot_b, part)
        dense = found if dense is None else dense + found
    wp_v[...] = dense[:, :LANES].reshape(CX, CY, LANES)
    gin_v[...] = mob_v[...] * dense[:, LANES:].reshape(CX, CY, LANES)

    inflow = jnp.sum(table, axis=0, keepdims=True)
    row_v[...] = jnp.broadcast_to(inflow, tile)
    rate = row_v[:, 32:64] - (cpp - 1.0) * row_v[:, 0:32]
    running = mm_full(rate, before_hot)
    well = base - friction[0] * running * jnp.abs(running)
    well_ref[...] = well[0:1]


def put(resid, lnphi, well, st, wp, gin, inj, resid_out, lnphi_out, well_out, done, sem):
    others = [
        pltpu.make_async_copy(lnphi, lnphi_out, sem.at[CX]),
        pltpu.make_async_copy(well, well_out, sem.at[CX + 1]),
    ]
    for copy in others:
        copy.start()
    planes = []
    for x in range(CX):
        for i in range(NC):
            v = inj[i]
            into = gin[x] * jnp.concatenate([v, v], axis=0)
            out = st[i, x + 1, pl.ds(8, CY), :] * wp[x]
            done[i, x] = resid[i, x] + (out + into)
        planes.append(pltpu.make_async_copy(done.at[:, x], resid_out.at[:, x], sem.at[x]))
        planes[-1].start()
    for copy in planes + others:
        copy.wait()


def per_device(n_grp, n_sub, *args):
    (
        amounts,
        pressure,
        heat,
        flag,
        perm,
        pore,
        former,
        trans,
        visc,
        crit,
        attract,
        covol,
        kappa,
        kij,
        recipe,
        locale,
        member,
        piece,
        strength,
        place,
        order,
        seg_pressure,
        exit_pressure,
        friction,
    ) = args
    field = (CX, CY, LANES)
    every = (NC, CX, CY, LANES)
    hbm = pl.BlockSpec(memory_space=pltpu.HBM)
    smem = pl.BlockSpec(memory_space=pltpu.SMEM)
    vmem = pl.BlockSpec(memory_space=pltpu.VMEM)
    mail = pltpu.VMEM((n_sub, 1, LANES), F32)
    one = pltpu.VMEM((8, LANES), F32)
    table = pltpu.VMEM((NC, 8, LANES), F32)
    edge = pltpu.VMEM((NC + 2, CX, LANES), F32)
    scratch = [
        pltpu.VMEM(every, F32),
        pltpu.VMEM(field, F32),
        pltpu.VMEM(field, jnp.int32),
        pltpu.VMEM(field, F32),
        pltpu.VMEM(every, F32),
        pltpu.VMEM(every, F32),
        pltpu.VMEM(every, F32),
        *[pltpu.VMEM(field, F32) for _ in range(11)],
        table,
        table,
        table,
        one,
        mail,
        mail,
        edge,
        edge,
        edge,
        edge,
        pltpu.SemaphoreType.DMA((8,)),
        pltpu.SemaphoreType.DMA,
        pltpu.SemaphoreType.DMA,
        pltpu.SemaphoreType.REGULAR((n_sub // LINE,)),
        pltpu.SemaphoreType.DMA((4,)),
        pltpu.SemaphoreType.DMA((4,)),
        pltpu.SemaphoreType.DMA((SMALL,)),
    ]
    small = (
        trans,
        visc,
        crit,
        attract,
        covol,
        kappa,
        kij,
        recipe,
        locale.reshape(2, LANES),
        member.reshape(2, LANES),
        piece.reshape(2, LANES),
        strength.reshape(2, LANES),
        place,
        order,
        seg_pressure,
    )
    spaces = [pltpu.SMEM] * SCALARS + [pltpu.VMEM] * (SMALL - SCALARS)
    held = [space(v.shape, v.dtype) for space, v in zip(spaces, small)]
    outs = (
        jax.ShapeDtypeStruct(every, F32),
        jax.ShapeDtypeStruct(every, BF16),
        jax.ShapeDtypeStruct((1, 32), F32),
    )
    found = pl.pallas_call(
        functools.partial(body, n_grp, n_sub),
        out_shape=(
            *outs,
            jax.ShapeDtypeStruct((NC + 2, CX + 2, CY + 16, LANES), F32),
            jax.ShapeDtypeStruct(field, F32),
            jax.ShapeDtypeStruct(field, F32),
            jax.ShapeDtypeStruct((NC, 8, LANES), F32),
        ),
        in_specs=[hbm] * (7 + SMALL) + [smem] * 2,
        out_specs=(vmem,) * 7,
        scratch_shapes=held + scratch,
        compiler_params=pltpu.CompilerParams(
            collective_id=0, has_side_effects=True, vmem_limit_bytes=40 * 1024 * 1024
        ),
        name="newton_residual",
    )(
        *[
            pltpu.with_memory_space_constraint(v, pltpu.HBM)
            for v in (amounts, pressure, heat, flag, perm, pore, former, *small)
        ],
        exit_pressure,
        friction,
    )
    return pl.pallas_call(
        put,
        out_shape=outs,
        in_specs=[vmem] * 7,
        out_specs=(hbm,) * 3,
        scratch_shapes=[pltpu.VMEM(every, F32), pltpu.SemaphoreType.DMA((CX + 2,))],
        compiler_params=pltpu.CompilerParams(vmem_limit_bytes=8 * 1024 * 1024),
        name="put_outputs",
    )(*found)


def solution(mesh):
    areal = P("grp", "sub", None)
    every = P(None, "grp", "sub", None)
    both = P(("grp", "sub"))
    rows = P(("grp", "sub"), None)
    in_specs = (
        every,
        areal,
        areal,
        areal,
        areal,
        areal,
        every,
        *[P()] * 8,
        both,
        rows,
        both,
        both,
        P("grp", None),
        rows,
        rows,
        both,
        both,
    )
    return jax.shard_map(
        functools.partial(per_device, mesh.shape["grp"], mesh.shape["sub"]),
        mesh=mesh,
        in_specs=in_specs,
        out_specs=(every, every, rows),
        check_vma=False,
    )
```
